128 devices in a mesh: freq: 8 (over x, z_hi), space: 16 (over z_lo, y, core).
Axes of the slice: x: 4, y: 4, z: 4 (z_hi: 2, z_lo: 2; z = z_hi * 2 + z_lo), core: 2. Of those that a mesh axis runs over, the one named last changes fastest.
Arguments:
- spectra: bfloat16 [128, 49152, 256], P('freq', 'space'), may hold values from -48 to 48, as said below
- weight: float32 [49152], P('space'), may hold values from 0.25 to 4
- partner: int32 [128], P('freq'), may hold values from 0 to 15
- counts: int32 [128], P('freq'), may hold values from 1 to 8
Outputs:
- modes: bfloat16 [128, 16, 49152], P('freq', None, 'space')
- energy: float32 [128, 8], P('freq')
- coherence: float32 [128, 2, 8, 8], P('freq')
The draws below stay inside these ranges and needn't reach their ends.
Inputs may be any that keep to these rules, and one draw needn't show every extreme that they name: spectra are finite Fourier coefficients.
All inputs are finite; a program needn't handle non-finite values.
Results may differ from the reference program's by a relative error of at most 0.0045.
Values may be sent and summed in bfloat16 or wider, within the bound.
No kernel may reach another device: no remote copies, remote signals or barrier semaphores. Data moves between devices by JAX's collectives and lax.ppermute only.
A program may use at most 128 MiB of HBM per device.

```python
import math
import jax
import jax.numpy as jnp
from jax import lax

NB = 128
FG = 16
KMAX = 8
ITERS = 4
NF = 128
NP = 49152
N_FREQ = 8


shared_terms = 256


def draw_spectra(key, part):
    keys = jax.random.split(key, 4)
    scales = jnp.exp(jax.random.uniform(keys[0], (NF, 1, NB), jnp.float32, 0.0, math.log(4.0)))
    noise = jax.random.normal(keys[1], (NF, NP, 2 * NB), jnp.float32)
    amplitude = 0.6
    shared = jax.random.normal(keys[2], (NP, shared_terms), jnp.float32)
    mixing = jax.random.normal(keys[3], (NF, shared_terms, 2 * NB), jnp.float32) * (amplitude * math.sqrt(8.0 / shared_terms))
    common = jnp.einsum('pr,frc->fpc', shared, mixing)
    doubled = jnp.concatenate([scales, scales], axis=2)
    return jnp.clip(doubled * (noise + common), -48.0, 48.0).astype(jnp.bfloat16)


def touch_ends(result, rng, low, high):
    place = [jax.random.randint(jax.random.fold_in(rng, axis), (), 0, length) for axis, length in enumerate(result.shape)]
    longest = result.shape.index(max(result.shape))
    beside = place[:longest] + [(place[longest] + 1) % result.shape[longest]] + place[longest + 1:]
    return result.at[tuple(place)].set(low).at[tuple(beside)].set(high)


def block_scale(rng, shape, cuts, smallest, high):
    loudness = 1.0
    for position, shards_of in cuts:
        heights = jax.random.uniform(jax.random.fold_in(jax.random.fold_in(rng, 6), position), (shards_of,), jnp.float32, smallest / len(cuts), high / len(cuts))
        loudness = loudness * jnp.repeat(jnp.exp(heights), shape[position] // shards_of).reshape((-1,) + (1,) * (len(shape) - 1 - position))
    return loudness


def setup_inputs(seed: int = 0) -> dict:
    arg_keys = jax.random.split(jax.random.key(seed), 5)
    return {
        "spectra": draw_spectra(jax.random.fold_in(arg_keys[4], 71), 0),
        "weight": jnp.clip(jnp.exp(math.log(4.0) - 2.7725887 * jax.random.uniform(arg_keys[1], (NP,), jnp.float32) ** block_scale(arg_keys[1], (NP,), ((0, 16),), -0.2, 0.2)), 0.25, 4.0),
        "partner": touch_ends(jax.random.randint(arg_keys[2], (NF,), 0, FG), jax.random.fold_in(arg_keys[2], 1), 0, FG - 1).astype(jnp.int32),
        "counts": touch_ends(jax.random.randint(arg_keys[3], (NF,), 1, KMAX + 1), jax.random.fold_in(arg_keys[3], 1), 1, KMAX).astype(jnp.int32),
    }


def embed(gram_re, gram_im):
    top = jnp.concatenate([gram_re, -gram_im], axis=2)
    bottom = jnp.concatenate([gram_im, gram_re], axis=2)
    return jnp.concatenate([top, bottom], axis=1)

def apply_operator(operator, basis):
    return jnp.einsum('fkc,fdc->fkd', basis, operator, precision=lax.Precision.HIGHEST)

def orthonormal(vectors, half):
    done = []
    for index in range(vectors.shape[1]):
        vector = vectors[:, index, :]
        for earlier in done:
            early_re, early_im = (earlier[:, :half], earlier[:, half:])
            vec_re, vec_im = (vector[:, :half], vector[:, half:])
            proj_re = lax.optimization_barrier(jnp.sum(early_re * vec_re + early_im * vec_im, axis=1, keepdims=True))
            proj_im = lax.optimization_barrier(jnp.sum(early_re * vec_im - early_im * vec_re, axis=1, keepdims=True))
            new_re = vec_re - proj_re * early_re + proj_im * early_im
            new_im = vec_im - proj_re * early_im - proj_im * early_re
            vector = jnp.concatenate([new_re, new_im], axis=1)
        length = jnp.sqrt(lax.optimization_barrier(jnp.sum(vector * vector, axis=1, keepdims=True)) + 1e-06)
        done.append(vector / length)
    return jnp.stack(done, axis=1)

def solve(gram_re, gram_im):
    half = gram_re.shape[1]
    operator = embed(gram_re, gram_im)
    basis = jnp.broadcast_to(jnp.eye(KMAX, 2 * half, dtype=jnp.float32), (gram_re.shape[0], KMAX, 2 * half))
    for sweep in range(ITERS):
        basis = orthonormal(apply_operator(operator, basis), half)
    image = apply_operator(operator, basis)
    energy = lax.optimization_barrier(jnp.sum(basis * image, axis=2))
    return (basis, energy)

def coefficients(basis, energy, counts):
    half = basis.shape[2] // 2
    ranks = jnp.arange(KMAX, dtype=jnp.int32)[None, :]
    scale = jnp.where(ranks < counts[:, None], 1.0 / jnp.sqrt(energy + 1e-06), 0.0)[:, :, None]
    part_re, part_im = (basis[:, :, :half], basis[:, :, half:])
    upper = jnp.concatenate([part_re, -part_im], axis=2) * scale
    lower = jnp.concatenate([part_im, part_re], axis=2) * scale
    return jnp.concatenate([upper, lower], axis=1).astype(jnp.bfloat16)

def reference(spectra, weight, partner, counts):
    half = NB

    def moment(block):
        weighted = (weight[:, None] * block).astype(jnp.bfloat16)
        return jnp.dot(block.T, weighted, preferred_element_type=jnp.float32)
    moments = lax.map(moment, spectra)
    gram_re = (moments[:, :half, :half] + moments[:, half:, half:]) / NP
    gram_im = (moments[:, :half, half:] - moments[:, half:, :half]) / NP
    basis, energy = solve(gram_re, gram_im)
    coefficient = coefficients(basis, energy, counts)

    def project(pair):
        return jnp.dot(pair[0], pair[1].T, preferred_element_type=jnp.float32).astype(jnp.bfloat16)
    modes = lax.map(project, (coefficient, spectra))
    freqs = jnp.arange(NF, dtype=jnp.int32)
    source = (N_FREQ - 1 - freqs // FG) * FG + partner
    partner_modes = jnp.take(modes, source.astype(jnp.int32), axis=0)

    def cohere(pair):
        phi = pair[0].astype(jnp.float32)
        psi = pair[1].astype(jnp.float32)
        wphi = phi * weight[None, :]
        hi = lax.Precision.HIGHEST
        real_part = jnp.dot(wphi[:KMAX], psi[:KMAX].T, precision=hi) + jnp.dot(wphi[KMAX:], psi[KMAX:].T, precision=hi)
        imag_part = jnp.dot(wphi[:KMAX], psi[KMAX:].T, precision=hi) - jnp.dot(wphi[KMAX:], psi[:KMAX].T, precision=hi)
        return jnp.stack([real_part, imag_part], axis=0) / NP
    coherence = lax.map(cohere, (modes, partner_modes))
    return (modes, energy, coherence)
```

```python
import functools

import jax
import jax.numpy as jnp
from jax import lax
from jax.experimental import pallas as pl
from jax.experimental.pallas import tpu as pltpu
from jax.sharding import PartitionSpec as P

KMAX = 8
ITERS = 4
EPS = 1e-06
F32 = jnp.float32
BF16 = jnp.bfloat16
VMEM = pl.BlockSpec(memory_space=pltpu.VMEM)
SMEM = pl.BlockSpec(memory_space=pltpu.SMEM)
ANY = pl.BlockSpec(memory_space=pl.ANY)


def kernel_params(**more):
    return pltpu.CompilerParams(vmem_limit_bytes=48 * 1024 * 1024, **more)


def cost(flops, moved):
    return pl.CostEstimate(flops=flops, bytes_accessed=moved, transcendentals=0)


def iotas(shape):
    return (
        lax.broadcasted_iota(jnp.int32, shape, 0),
        lax.broadcasted_iota(jnp.int32, shape, 1),
    )


def gram_kernel(slots, per_step, spectra, weight, packed, held, sems):
    groups, points, width = spectra.shape
    half = width // 2
    steps = groups // per_step
    rows, cols = iotas((half, half))

    def fetch(step, slot):
        return pltpu.make_async_copy(
            spectra.at[pl.ds(step * per_step, per_step)], held.at[slot], sems.at[slot]
        )

    for slot in range(slots):
        fetch(slot, slot).start()

    def body(step, carry):
        slot = lax.rem(step, slots)
        fetch(step, slot).wait()
        for index in range(per_step):
            block = held[slot, index]
            weighted = (block.T.astype(F32) * weight[...]).astype(BF16)
            moment = jnp.dot(weighted, block, preferred_element_type=F32)
            real = moment[:half, :half] + moment[half:, half:]
            imag = moment[:half, half:] - moment[half:, :half]
            packed[step * per_step + index] = jnp.where(cols >= rows, real, imag).astype(BF16)

        @pl.when(step + slots < steps)
        def _():
            fetch(step + slots, slot).start()

        return carry

    lax.fori_loop(0, steps, body, 0)


def gram(spectra, weight):
    groups, points, width = spectra.shape
    half = width // 2
    slots, per_step = (4, 2)
    return pl.pallas_call(
        functools.partial(gram_kernel, slots, per_step),
        in_specs=[ANY, VMEM],
        out_specs=VMEM,
        out_shape=jax.ShapeDtypeStruct((groups, half, half), BF16),
        scratch_shapes=[
            pltpu.VMEM((slots, per_step, points, width), BF16),
            pltpu.SemaphoreType.DMA((slots,)),
        ],
        compiler_params=kernel_params(),
        cost_estimate=cost(2 * groups * points * width * width, groups * points * width * 2),
        name="gram",
    )(spectra, weight)


def orthonormal(re, im):
    rows, _ = iotas(re.shape)
    for k in range(KMAX):
        ure = jnp.broadcast_to(re[k : k + 1], re.shape)
        uim = jnp.broadcast_to(im[k : k + 1], im.shape)
        square = jnp.sum(ure * ure + uim * uim, axis=1, keepdims=True) + EPS
        pre = jnp.sum(ure * re + uim * im, axis=1, keepdims=True)
        pim = jnp.sum(ure * im - uim * re, axis=1, keepdims=True)
        inverse = 1.0 / square
        pre = pre * inverse
        pim = pim * inverse
        unit = 1.0 / jnp.sqrt(square)
        re, im = (
            jnp.where(rows > k, re - pre * ure + pim * uim, jnp.where(rows == k, ure * unit, re)),
            jnp.where(rows > k, im - pre * uim - pim * ure, jnp.where(rows == k, uim * unit, im)),
        )
    return (re, im)


def solve_kernel(total, parts, counts, out):
    count, half, _ = parts.shape
    summed = parts[0].astype(F32)
    for index in range(1, count):
        summed = summed + parts[index].astype(F32)
    summed = summed / total
    flipped = summed.T
    rows, cols = iotas((half, half))
    gram_re = jnp.where(cols >= rows, summed, flipped)
    gram_im = jnp.where(cols < rows, summed, jnp.where(cols > rows, -flipped, 0.0))
    operator = jnp.concatenate(
        [
            jnp.concatenate([gram_re, -gram_im], axis=1),
            jnp.concatenate([gram_im, gram_re], axis=1),
        ],
        axis=0,
    )
    high = operator.astype(BF16)
    low = (operator - high.astype(F32)).astype(BF16)

    def apply(re, im):
        vectors = jnp.concatenate([re, im], axis=1)
        vhigh = vectors.astype(BF16)
        vlow = (vectors - vhigh.astype(F32)).astype(BF16)
        both = jnp.concatenate([vhigh, vlow], axis=0)
        first = jnp.dot(both, high, preferred_element_type=F32)
        second = jnp.dot(both, low, preferred_element_type=F32)
        image = first[:KMAX] + first[KMAX:] + second[:KMAX]
        return (image[:, :half], image[:, half:])

    re, im = orthonormal(gram_re[:KMAX], -gram_im[:KMAX])
    for _ in range(ITERS - 1):
        re, im = orthonormal(*apply(re, im))
    image_re, image_im = apply(re, im)
    energy = jnp.sum(re * image_re + im * image_im, axis=1, keepdims=True)
    kept = counts[lax.axis_index("space")]
    ranks, lanes = iotas((KMAX, half))
    scale = jnp.where(ranks[:, :1] < kept, 1.0 / jnp.sqrt(energy + EPS), 0.0)
    first = energy.astype(BF16)
    rest = energy - first.astype(F32)
    second = rest.astype(BF16)
    third = (rest - second.astype(F32)).astype(BF16)
    tail = jnp.where(
        lanes == 0,
        first.astype(F32),
        jnp.where(lanes == 1, second.astype(F32), jnp.where(lanes == 2, third.astype(F32), 0.0)),
    )
    message = jnp.concatenate([re * scale, im * scale, tail], axis=1).astype(BF16)
    for index in range(out.shape[0]):
        out[index] = message


def solve(parts, counts, total):
    count, half, _ = parts.shape
    return pl.pallas_call(
        functools.partial(solve_kernel, total),
        in_specs=[VMEM, SMEM],
        out_specs=VMEM,
        out_shape=jax.ShapeDtypeStruct((count, KMAX, 3 * half), BF16),
        compiler_params=kernel_params(),
        cost_estimate=cost(8_000_000_000, parts.size * 2),
        name="solve",
    )(parts, counts)


def coefficient_rows(message, half):
    part_re = message[:, :half]
    part_im = message[:, half : 2 * half]
    return jnp.concatenate(
        [
            jnp.concatenate([part_re, -part_im], axis=1),
            jnp.concatenate([part_im, part_re], axis=1),
        ],
        axis=0,
    )


def project(rows, block):
    return lax.dot_general(
        rows, block, (((1,), (1,)), ((), ())), preferred_element_type=F32
    ).astype(BF16)


def part_kernel(begin, size, half_index, messages, spectra, out, held, sems):
    groups, points, width = spectra.shape
    start = pl.multiple_of(half_index[0] * (points // 2) + begin, 128)
    copies = [
        pltpu.make_async_copy(
            spectra.at[index, pl.ds(start, size)], held.at[index], sems.at[index]
        )
        for index in range(groups)
    ]
    for copy in copies:
        copy.start()
    for index in range(groups):
        copies[index].wait()
        out[index] = project(coefficient_rows(messages[index], width // 2), held[index])


def modes_part(half_index, messages, spectra, begin, size):
    groups, points, width = spectra.shape
    return pl.pallas_call(
        functools.partial(part_kernel, begin, size),
        in_specs=[SMEM, VMEM, ANY],
        out_specs=VMEM,
        out_shape=jax.ShapeDtypeStruct((groups, 2 * KMAX, size), BF16),
        scratch_shapes=[
            pltpu.VMEM((groups, size, width), BF16),
            pltpu.SemaphoreType.DMA((groups,)),
        ],
        compiler_params=kernel_params(),
        cost_estimate=cost(2_000_000_000, groups * size * width * 2),
        name="modes_part",
    )(half_index, messages, spectra)


def modes_kernel(slots, keep, messages, weight, spectra, out, high, low, held, made, sems, put):
    groups, points, width = spectra.shape
    part = points // 2
    start = pl.multiple_of(keep[0] * part, 128)

    def fetch(step, slot):
        return pltpu.make_async_copy(spectra.at[step], held.at[slot], sems.at[slot])

    def store(step, slot):
        return pltpu.make_async_copy(made.at[slot], out.at[step], put.at[slot])

    for slot in range(slots):
        fetch(slot, slot).start()

    def body(step, carry):
        slot = lax.rem(step, slots)

        @pl.when(step >= slots)
        def _():
            store(step - slots, slot).wait()

        fetch(step, slot).wait()
        made[slot] = project(coefficient_rows(messages[step], width // 2), held[slot])
        store(step, slot).start()
        own = made[slot, :, pl.ds(start, part)].astype(F32) * weight[:, pl.ds(start, part)]
        top = own.astype(BF16)
        high[step] = top
        low[step] = (own - top.astype(F32)).astype(BF16)

        @pl.when(step + slots < groups)
        def _():
            fetch(step + slots, slot).start()

        return carry

    lax.fori_loop(0, groups, body, 0)
    for slot in range(slots):
        store(groups - slots + slot, slot).wait()


def modes_all(keep, messages, weight, spectra):
    groups, points, width = spectra.shape
    slots = 4
    weighted = jax.ShapeDtypeStruct((groups, 2 * KMAX, points // 2), BF16)
    return pl.pallas_call(
        functools.partial(modes_kernel, slots),
        in_specs=[SMEM, VMEM, VMEM, ANY],
        out_specs=(ANY, VMEM, VMEM),
        out_shape=(
            jax.ShapeDtypeStruct((groups, 2 * KMAX, points), BF16),
            weighted,
            weighted,
        ),
        scratch_shapes=[
            pltpu.VMEM((slots, points, width), BF16),
            pltpu.VMEM((slots, 2 * KMAX, points), BF16),
            pltpu.SemaphoreType.DMA((slots,)),
            pltpu.SemaphoreType.DMA((slots,)),
        ],
        compiler_params=kernel_params(),
        cost_estimate=cost(10_000_000_000, groups * points * width * 2),
        name="modes_all",
    )(keep, messages, weight, spectra)


def chosen(cross, lane_partner, groups):
    rank = 2 * KMAX
    top = jnp.zeros((KMAX, groups * rank), F32)
    bottom = jnp.zeros((KMAX, groups * rank), F32)
    for index in range(groups):
        taken = lane_partner == index
        top = jnp.where(taken, cross[index * rank : index * rank + KMAX], top)
        bottom = jnp.where(taken, cross[index * rank + KMAX : (index + 1) * rank], bottom)
    _, lanes = iotas(top.shape)
    width = groups * rank
    return jnp.where(
        lanes % rank < KMAX,
        top + pltpu.roll(bottom, width - KMAX, 1),
        pltpu.roll(bottom, KMAX, 1) - top,
    )


def cross_kernel(first_mine, own_partner, other_partner, high, low, *rest):
    arrived, out = (rest[:-1], rest[-1])
    groups, rank, part = high.shape
    rows = groups * rank
    cross = jnp.zeros((rows, rows), F32)
    begin = 0
    for share in arrived:
        size = share.shape[2]
        other = share[...].reshape(rows, size)
        for own in (high, low):
            mine = own[:, :, begin : begin + size].reshape(rows, size)
            cross = cross + lax.dot_general(
                mine, other, (((1,), (1,)), ((), ())), preferred_element_type=F32
            )
        begin += size
    own_value = chosen(cross.T, own_partner[...], groups).astype(BF16)
    other_value = chosen(cross, other_partner[...], groups).astype(BF16)
    mine_first = first_mine[0] == 1
    half = out.shape[0] // 2
    lower = jnp.where(mine_first, own_value, other_value)
    upper = jnp.where(mine_first, other_value, own_value)
    for index in range(half):
        out[index] = lower
        out[half + index] = upper


def cross_sums(first_mine, own_partner, other_partner, high, low, arrived, members):
    groups, rank, part = high.shape
    return pl.pallas_call(
        cross_kernel,
        in_specs=[SMEM] + [VMEM] * (4 + len(arrived)),
        out_specs=VMEM,
        out_shape=jax.ShapeDtypeStruct((members, KMAX, groups * rank), BF16),
        compiler_params=kernel_params(),
        cost_estimate=cost(2_000_000_000, 4 * high.size),
        name="cross_sums",
    )(first_mine, own_partner, other_partner, high, low, *arrived)


def finish_kernel(total, parts, out):
    summed = parts[0].astype(F32)
    for index in range(1, parts.shape[0]):
        summed = summed + parts[index].astype(F32)
    out[...] = (summed / total).T


def finish(parts, total):
    _, kmax, width = parts.shape
    return pl.pallas_call(
        functools.partial(finish_kernel, total),
        in_specs=[VMEM],
        out_specs=VMEM,
        out_shape=jax.ShapeDtypeStruct((width, kmax), F32),
        compiler_params=kernel_params(),
        cost_estimate=cost(1_000_000, parts.size * 2),
        name="finish",
    )(parts)


def on_device(spectra, weight, partner, counts):
    groups, points, width = spectra.shape
    n_freq, n_space = (lax.axis_size("freq"), lax.axis_size("space"))
    total = points * n_space
    place = lax.axis_index("freq")
    lower_group = place < n_freq // 2
    keep = jnp.where(lower_group, 0, 1).astype(jnp.int32).reshape(1)
    give = 1 - keep
    weight_row = weight[None, :]
    lane_partner = jnp.repeat(partner, 2 * KMAX)[None, :]
    mirror = [(index, n_freq - 1 - index) for index in range(n_freq)]

    packed = gram(spectra, weight_row)
    parts = lax.all_to_all(packed, "space", 0, 0, tiled=True)
    message = solve(parts, counts, total)
    messages = lax.all_to_all(message, "space", 0, 0, tiled=True)

    pieces = 2
    size = points // 2 // pieces
    shares = [
        modes_part(give, messages, spectra, index * size, size) for index in range(pieces)
    ]
    arrived = [lax.ppermute(share, "freq", mirror) for share in shares]
    other_partner = lax.ppermute(lane_partner, "freq", mirror)
    modes, high, low = modes_all(keep, messages, weight_row, spectra)
    energy = jnp.sum(messages[:, :, width : width + 3].astype(F32), axis=2)

    pairs = [
        [group * n_space + index for group in (low_group, n_freq - 1 - low_group) for index in range(n_space)]
        for low_group in range(n_freq // 2)
    ]
    sums = cross_sums(
        give, lane_partner, other_partner, high, low, arrived, 2 * n_space
    )
    gathered = lax.all_to_all(
        sums, ("freq", "space"), 0, 0, tiled=True, axis_index_groups=pairs
    )
    coherence = finish(gathered, total).reshape(groups, 2, KMAX, KMAX)
    return (modes, energy, coherence)


def solution(mesh):
    in_specs = (P("freq", "space", None), P("space"), P("freq"), P("freq"))
    out_specs = (P("freq", None, "space"), P("freq", None), P("freq", None, None, None))
    return jax.shard_map(
        on_device, mesh=mesh, in_specs=in_specs, out_specs=out_specs, check_vma=False
    )
```

```python
import functools

import jax
import jax.numpy as jnp
from jax import lax
from jax.experimental import pallas as pl
from jax.experimental.pallas import tpu as pltpu
from jax.sharding import PartitionSpec as P

KMAX = 8
ITERS = 4
EPS = 1e-06
F32 = jnp.float32
BF16 = jnp.bfloat16
VMEM = pl.BlockSpec(memory_space=pltpu.VMEM)
SMEM = pl.BlockSpec(memory_space=pltpu.SMEM)
ANY = pl.BlockSpec(memory_space=pl.ANY)
HBM = pl.BlockSpec(memory_space=pltpu.HBM)


def kernel_params(mebibytes):
    return pltpu.CompilerParams(vmem_limit_bytes=mebibytes * 1024 * 1024)


def cost(flops, moved):
    return pl.CostEstimate(flops=flops, bytes_accessed=moved, transcendentals=0)


def kept_half():
    return jnp.where(lax.axis_index("freq") < lax.axis_size("freq") // 2, 0, 1)


def iotas(shape):
    return (
        lax.broadcasted_iota(jnp.int32, shape, 0),
        lax.broadcasted_iota(jnp.int32, shape, 1),
    )


def gram_kernel(depth, spectra, weight, packed, held, scale, sems, scale_sem):
    groups, points, width = spectra.shape
    half = width // 2
    slots, per_step = held.shape[:2]
    steps = groups // per_step
    rows, cols = iotas((half, half))

    def fetch(step):
        slot = lax.rem(step, slots)
        return pltpu.make_async_copy(
            spectra.at[pl.ds(step * per_step, per_step)], held.at[slot], sems.at[slot]
        )

    fetch(0).start()
    scale_copy = pltpu.make_async_copy(weight, scale, scale_sem)
    scale_copy.start()
    for step in range(1, depth):
        fetch(step).start()
    scale_copy.wait()

    def body(step, carry):
        fetch(step).wait()

        @pl.when(step + depth < steps)
        def _():
            fetch(step + depth).start()

        for index in range(per_step):
            block = held[lax.rem(step, slots), index]
            weighted = (block.T.astype(F32) * scale[...]).astype(BF16)
            moment = jnp.dot(weighted, block, preferred_element_type=F32)
            real = moment[:half, :half] + moment[half:, half:]
            imag = moment[:half, half:] - moment[half:, :half]
            packed[step * per_step + index] = jnp.where(cols >= rows, real, imag).astype(BF16)
        return carry

    lax.fori_loop(0, steps, body, 0)


def gram(spectra, weight):
    groups, points, width = spectra.shape
    half = width // 2
    depth, slots, per_step = (2, 3, 2)
    return pl.pallas_call(
        functools.partial(gram_kernel, depth),
        in_specs=[HBM, ANY],
        out_specs=VMEM,
        out_shape=jax.ShapeDtypeStruct((groups, half, half), BF16),
        scratch_shapes=[
            pltpu.VMEM((slots, per_step, points, width), BF16),
            pltpu.VMEM((1, points), F32),
            pltpu.SemaphoreType.DMA((slots,)),
            pltpu.SemaphoreType.DMA,
        ],
        compiler_params=kernel_params(24),
        cost_estimate=cost(2 * groups * points * width * width, groups * points * width * 2),
        name="gram",
    )(spectra, weight)


def orthonormal(re, im):
    rows, _ = iotas(re.shape)
    for k in range(KMAX):
        ure = jnp.broadcast_to(re[k : k + 1], re.shape)
        uim = jnp.broadcast_to(im[k : k + 1], im.shape)
        square = jnp.sum(ure * ure + uim * uim, axis=1, keepdims=True) + EPS
        pre = jnp.sum(ure * re + uim * im, axis=1, keepdims=True)
        pim = jnp.sum(ure * im - uim * re, axis=1, keepdims=True)
        inverse = 1.0 / square
        pre = pre * inverse
        pim = pim * inverse
        unit = 1.0 / jnp.sqrt(square)
        re, im = (
            jnp.where(rows > k, re - pre * ure + pim * uim, jnp.where(rows == k, ure * unit, re)),
            jnp.where(rows > k, im - pre * uim - pim * ure, jnp.where(rows == k, uim * unit, im)),
        )
    return (re, im)


def solve_kernel(total, parts, counts, spectra, out, staged, sems):
    count, half, _ = parts.shape
    groups, part, _ = staged.shape
    start = pl.multiple_of((1 - kept_half()) * part, 128)
    copies = [
        pltpu.make_async_copy(
            spectra.at[index, pl.ds(start, part)], staged.at[index], sems.at[index]
        )
        for index in range(groups)
    ]
    for copy in copies:
        copy.start()
    summed = parts[0].astype(F32)
    for index in range(1, count):
        summed = summed + parts[index].astype(F32)
    summed = summed / total
    flipped = summed.T
    rows, cols = iotas((half, half))
    gram_re = jnp.where(cols >= rows, summed, flipped)
    gram_im = jnp.where(cols < rows, summed, jnp.where(cols > rows, -flipped, 0.0))
    operator = jnp.concatenate(
        [
            jnp.concatenate([gram_re, -gram_im], axis=1),
            jnp.concatenate([gram_im, gram_re], axis=1),
        ],
        axis=0,
    )
    high = operator.astype(BF16)
    low = (operator - high.astype(F32)).astype(BF16)

    def apply(re, im):
        vectors = jnp.concatenate([re, im], axis=1)
        vhigh = vectors.astype(BF16)
        vlow = (vectors - vhigh.astype(F32)).astype(BF16)
        both = jnp.concatenate([vhigh, vlow], axis=0)
        first = jnp.dot(both, high, preferred_element_type=F32)
        second = jnp.dot(both, low, preferred_element_type=F32)
        image = first[:KMAX] + first[KMAX:] + second[:KMAX]
        return (image[:, :half], image[:, half:])

    re, im = orthonormal(gram_re[:KMAX], -gram_im[:KMAX])
    for _ in range(ITERS - 1):
        re, im = orthonormal(*apply(re, im))
    image_re, image_im = apply(re, im)
    energy = jnp.sum(re * image_re + im * image_im, axis=1, keepdims=True)
    kept = counts[lax.axis_index("space")]
    ranks, lanes = iotas((KMAX, half))
    scale = jnp.where(ranks[:, :1] < kept, 1.0 / jnp.sqrt(energy + EPS), 0.0)
    first = energy.astype(BF16)
    rest = energy - first.astype(F32)
    second = rest.astype(BF16)
    third = (rest - second.astype(F32)).astype(BF16)
    tail = jnp.where(
        lanes == 0,
        first.astype(F32),
        jnp.where(lanes == 1, second.astype(F32), jnp.where(lanes == 2, third.astype(F32), 0.0)),
    )
    message = jnp.concatenate([re * scale, im * scale, tail], axis=1).astype(BF16)
    for index in range(out.shape[0]):
        out[index] = message
    for copy in copies:
        copy.wait()


def solve(parts, counts, spectra, total):
    count, half, _ = parts.shape
    groups, points, width = spectra.shape
    return pl.pallas_call(
        functools.partial(solve_kernel, total),
        in_specs=[VMEM, SMEM, HBM],
        out_specs=(VMEM, VMEM),
        out_shape=(
            jax.ShapeDtypeStruct((count, KMAX, 3 * half), BF16),
            pltpu.VMEM((groups, points // 2, width), BF16),
        ),
        scratch_shapes=[pltpu.SemaphoreType.DMA((groups,))],
        compiler_params=kernel_params(16),
        cost_estimate=cost(8_000_000_000, groups * points * width),
        name="solve",
    )(parts, counts, spectra)


def coefficient_rows(message, half):
    part_re = message[:, :half]
    part_im = message[:, half : 2 * half]
    return jnp.concatenate(
        [
            jnp.concatenate([part_re, -part_im], axis=1),
            jnp.concatenate([part_im, part_re], axis=1),
        ],
        axis=0,
    )


def project(rows, block):
    return lax.dot_general(
        rows, block, (((1,), (1,)), ((), ())), preferred_element_type=F32
    ).astype(BF16)


def part_kernel(begin, size, messages, staged, *rest):
    out = rest[-1]
    groups, _, width = staged.shape
    for index in range(groups):
        rows = coefficient_rows(messages[index], width // 2)
        out[index] = project(rows, staged[index, begin : begin + size])


def modes_part(messages, staged, begin, size, *after):
    groups, _, width = staged.shape
    return pl.pallas_call(
        functools.partial(part_kernel, begin, size),
        in_specs=[VMEM, VMEM] + [ANY] * len(after),
        out_specs=VMEM,
        out_shape=jax.ShapeDtypeStruct((groups, 2 * KMAX, size), BF16),
        compiler_params=kernel_params(8),
        cost_estimate=cost(2_000_000_000, groups * size * width * 2),
        name="modes_part",
    )(messages, staged, *after)


def modes_kernel(slots, messages, weight, spectra, out, energy, high, low, held, made, sems, put):
    groups, points, width = spectra.shape
    part = points // 2
    start = pl.multiple_of(kept_half() * part, 128)

    def fetch(step, slot):
        return pltpu.make_async_copy(spectra.at[step], held.at[slot], sems.at[slot])

    def store(step, slot):
        return pltpu.make_async_copy(made.at[slot], out.at[step], put.at[slot])

    for slot in range(slots):
        fetch(slot, slot).start()
    _, lanes = iotas(energy.shape)
    value = jnp.zeros(energy.shape, F32)
    for index in range(groups):
        column = jnp.sum(messages[index, :, width:].astype(F32), axis=1, keepdims=True)
        value = jnp.where(lanes == index, column, value)
    energy[...] = value

    def body(step, carry):
        slot = lax.rem(step, slots)

        @pl.when(step >= slots)
        def _():
            store(step - slots, slot).wait()

        fetch(step, slot).wait()
        made[slot] = project(coefficient_rows(messages[step], width // 2), held[slot])
        store(step, slot).start()
        own = made[slot, :, pl.ds(start, part)].astype(F32) * weight[:, pl.ds(start, part)]
        top = own.astype(BF16)
        high[step] = top
        low[step] = (own - top.astype(F32)).astype(BF16)

        @pl.when(step + slots < groups)
        def _():
            fetch(step + slots, slot).start()

        return carry

    lax.fori_loop(0, groups, body, 0)
    for slot in range(slots):
        store(groups - slots + slot, slot).wait()


def modes_all(messages, weight, spectra):
    groups, points, width = spectra.shape
    slots = 4
    weighted = jax.ShapeDtypeStruct((groups, 2 * KMAX, points // 2), BF16)
    return pl.pallas_call(
        functools.partial(modes_kernel, slots),
        in_specs=[VMEM, VMEM, HBM],
        out_specs=(HBM, VMEM, VMEM, VMEM),
        out_shape=(
            jax.ShapeDtypeStruct((groups, 2 * KMAX, points), BF16),
            jax.ShapeDtypeStruct((KMAX, groups), F32),
            weighted,
            weighted,
        ),
        scratch_shapes=[
            pltpu.VMEM((slots, points, width), BF16),
            pltpu.VMEM((slots, 2 * KMAX, points), BF16),
            pltpu.SemaphoreType.DMA((slots,)),
            pltpu.SemaphoreType.DMA((slots,)),
        ],
        compiler_params=kernel_params(24),
        cost_estimate=cost(10_000_000_000, groups * points * width * 2),
        name="modes_all",
    )(messages, weight, spectra)


def lane_table(partner, rank):
    groups = partner.shape[0]
    _, lanes = iotas((KMAX, groups * rank))
    table = jnp.zeros((KMAX, groups * rank), jnp.int32)
    for index in range(groups):
        table = jnp.where(lanes // rank == index, partner[index], table)
    return table


def chosen(cross, lane_partner, groups):
    rank = 2 * KMAX
    top = jnp.zeros((KMAX, groups * rank), F32)
    bottom = jnp.zeros((KMAX, groups * rank), F32)
    for index in range(groups):
        taken = lane_partner == index
        top = jnp.where(taken, cross[index * rank : index * rank + KMAX], top)
        bottom = jnp.where(taken, cross[index * rank + KMAX : (index + 1) * rank], bottom)
    _, lanes = iotas(top.shape)
    width = groups * rank
    return jnp.where(
        lanes % rank < KMAX,
        top + pltpu.roll(bottom, width - KMAX, 1),
        pltpu.roll(bottom, KMAX, 1) - top,
    )


def cross_kernel(own_partner, other_partner, high, low, *rest):
    arrived, out = (rest[:-1], rest[-1])
    groups, rank, part = high.shape
    rows = groups * rank
    cross = jnp.zeros((rows, rows), F32)
    begin = 0
    for share in arrived:
        size = share.shape[2]
        other = share[...].reshape(rows, size)
        for own in (high, low):
            mine = own[:, :, begin : begin + size].reshape(rows, size)
            cross = cross + lax.dot_general(
                mine, other, (((1,), (1,)), ((), ())), preferred_element_type=F32
            )
        begin += size
    out[:KMAX] = chosen(cross.T, lane_table(own_partner, rank), groups)
    out[KMAX:] = chosen(cross, lane_table(other_partner, rank), groups)


def cross_sums(own_partner, other_partner, high, low, arrived):
    groups, rank, part = high.shape
    return pl.pallas_call(
        cross_kernel,
        in_specs=[SMEM, SMEM] + [VMEM] * (2 + len(arrived)),
        out_specs=VMEM,
        out_shape=jax.ShapeDtypeStruct((2 * KMAX, groups * rank), F32),
        compiler_params=kernel_params(16),
        cost_estimate=cost(2_000_000_000, 4 * high.size),
        name="cross_sums",
    )(own_partner, other_partner, high, low, *arrived)


def spread_kernel(mine, other, out):
    summed = (mine[...] + other[...]).astype(BF16)
    width = summed.shape[1]
    rank = 2 * KMAX
    rows, cols = iotas((width, width))
    moved = cols == (rows % rank) * (width // rank) + rows // rank
    ordered = jnp.dot(summed, moved.astype(F32).astype(BF16), preferred_element_type=F32)
    first = kept_half() == 0
    lower = jnp.where(first, ordered[:KMAX], ordered[KMAX:]).astype(BF16)
    upper = jnp.where(first, ordered[KMAX:], ordered[:KMAX]).astype(BF16)
    half = out.shape[0] // 2
    for index in range(half):
        out[index] = lower
        out[half + index] = upper


def spread(mine, other, members):
    return pl.pallas_call(
        spread_kernel,
        in_specs=[VMEM, VMEM],
        out_specs=VMEM,
        out_shape=jax.ShapeDtypeStruct((members, KMAX, mine.shape[1]), BF16),
        compiler_params=kernel_params(8),
        cost_estimate=cost(10_000_000, 4 * mine.size),
        name="spread",
    )(mine, other)


def finish_kernel(total, parts, out):
    summed = parts[0].astype(F32)
    for index in range(1, parts.shape[0]):
        summed = summed + parts[index].astype(F32)
    summed = summed / total
    groups = out.shape[3]
    for side in range(2):
        for k in range(KMAX):
            begin = (side * KMAX + k) * groups
            out[side, k] = summed[:, begin : begin + groups]


def finish(parts, total):
    _, kmax, width = parts.shape
    return pl.pallas_call(
        functools.partial(finish_kernel, total),
        in_specs=[VMEM],
        out_specs=VMEM,
        out_shape=jax.ShapeDtypeStruct((2, kmax, kmax, width // (2 * kmax)), F32),
        compiler_params=kernel_params(8),
        cost_estimate=cost(1_000_000, parts.size * 2),
        name="finish",
    )(parts)


def on_device(spectra, weight, partner, counts):
    groups, points, width = spectra.shape
    n_freq, n_space = (lax.axis_size("freq"), lax.axis_size("space"))
    total = points * n_space
    spectra = pltpu.with_memory_space_constraint(spectra, pltpu.HBM)
    weight_row = weight[None, :]
    mirror = [(index, n_freq - 1 - index) for index in range(n_freq)]

    packed = gram(spectra, pltpu.with_memory_space_constraint(weight_row, pltpu.HBM))
    parts = lax.all_to_all(packed, "space", 0, 0, tiled=True)
    message, staged = solve(parts, counts, spectra, total)
    messages = lax.all_to_all(message, "space", 0, 0, tiled=True)

    staged = pltpu.with_memory_space_constraint(staged, pltpu.VMEM)
    part = points // 2
    cut = part // 4
    first_share = modes_part(messages, staged, 0, cut)
    shares = [first_share, modes_part(messages, staged, cut, part - cut, first_share)]
    arrived = [lax.ppermute(share, "freq", mirror) for share in shares]
    later_partner, _ = lax.optimization_barrier((partner, shares[-1]))
    other_partner = lax.ppermute(later_partner, "freq", mirror)
    modes, energy, high, low = modes_all(messages, weight_row, spectra)

    sums = cross_sums(partner, other_partner, high, low, arrived)
    paired = lax.ppermute(sums, "space", [(index, index ^ 1) for index in range(n_space)])
    members = [
        [group * n_space + index for group in (low_group, n_freq - 1 - low_group) for index in range(core, n_space, 2)]
        for low_group in range(n_freq // 2)
        for core in range(2)
    ]
    gathered = lax.all_to_all(
        spread(sums, paired, n_space),
        ("freq", "space"),
        0,
        0,
        tiled=True,
        axis_index_groups=members,
    )
    coherence = jnp.transpose(finish(gathered, total), (3, 0, 1, 2))
    return (modes, jnp.transpose(energy), coherence)


def solution(mesh):
    in_specs = (P("freq", "space", None), P("space"), P("freq"), P("freq"))
    out_specs = (P("freq", None, "space"), P("freq", None), P("freq", None, None, None))
    return jax.shard_map(
        on_device, mesh=mesh, in_specs=in_specs, out_specs=out_specs, check_vma=False
    )
```

```python
import functools

import jax
import jax.numpy as jnp
from jax import lax
from jax.experimental import pallas as pl
from jax.experimental.pallas import tpu as pltpu
from jax.sharding import PartitionSpec as P

KMAX = 8
ITERS = 4
EPS = 1e-06
F32 = jnp.float32
BF16 = jnp.bfloat16
VMEM = pl.BlockSpec(memory_space=pltpu.VMEM)
SMEM = pl.BlockSpec(memory_space=pltpu.SMEM)
ANY = pl.BlockSpec(memory_space=pl.ANY)
HBM = pl.BlockSpec(memory_space=pltpu.HBM)


def kernel_params(mebibytes):
    return pltpu.CompilerParams(vmem_limit_bytes=mebibytes * 1024 * 1024)


def cost(flops, moved):
    return pl.CostEstimate(flops=flops, bytes_accessed=moved, transcendentals=0)


def kept_half():
    return jnp.where(lax.axis_index("freq") < lax.axis_size("freq") // 2, 0, 1)


def iotas(shape):
    return (
        lax.broadcasted_iota(jnp.int32, shape, 0),
        lax.broadcasted_iota(jnp.int32, shape, 1),
    )


def gram_kernel(depth, per_step, spectra, weight, mine, other, resident, scale, sems, scale_sem):
    groups, points, width = spectra.shape
    half = width // 2
    steps = groups // per_step
    rows, cols = iotas((half, half))
    south = lax.rem(lax.axis_index("space"), 2) == 0

    def fetch(step):
        part = pl.ds(step * per_step, per_step)
        return pltpu.make_async_copy(spectra.at[part], resident.at[part], sems.at[step])

    fetch(0).start()
    scale_copy = pltpu.make_async_copy(weight, scale, scale_sem)
    scale_copy.start()
    for step in range(1, depth):
        fetch(step).start()
    scale_copy.wait()

    def hermitian(index):
        block = resident[index]
        weighted = (block.T.astype(F32) * scale[...]).astype(BF16)
        moment = jnp.dot(weighted, block, preferred_element_type=F32)
        real = moment[:half, :half] + moment[half:, half:]
        imag = moment[:half, half:] - moment[half:, :half]
        return jnp.where(cols >= rows, real, imag)

    def body(step, carry):
        fetch(step).wait()

        @pl.when(step + depth < steps)
        def _():
            fetch(step + depth).start()

        for index in range(0, per_step, 2):
            even = hermitian(step * per_step + index)
            odd = hermitian(step * per_step + index + 1)
            place = (step * per_step + index) // 2
            mine[place] = jnp.where(south, even, odd)
            other[place] = jnp.where(south, odd, even)
        return carry

    lax.fori_loop(0, steps, body, 0)


def gram(spectra, weight):
    groups, points, width = spectra.shape
    half = width // 2
    depth, per_step = (2, 2)
    sums = jax.ShapeDtypeStruct((groups // 2, half, half), F32)
    return pl.pallas_call(
        functools.partial(gram_kernel, depth, per_step),
        in_specs=[HBM, HBM],
        out_specs=(VMEM, VMEM, VMEM),
        out_shape=(sums, sums, pltpu.VMEM((groups, points, width), BF16)),
        scratch_shapes=[
            pltpu.VMEM((1, points), F32),
            pltpu.SemaphoreType.DMA((groups // per_step,)),
            pltpu.SemaphoreType.DMA,
        ],
        compiler_params=kernel_params(16),
        cost_estimate=cost(2 * groups * points * width * width, groups * points * width * 2),
        name="gram",
    )(spectra, weight)


def orthonormal(re, im):
    rows, _ = iotas(re.shape)
    for k in range(KMAX):
        ure = jnp.broadcast_to(re[k : k + 1], re.shape)
        uim = jnp.broadcast_to(im[k : k + 1], im.shape)
        square = jnp.sum(ure * ure + uim * uim, axis=1, keepdims=True) + EPS
        pre = jnp.sum(ure * re + uim * im, axis=1, keepdims=True)
        pim = jnp.sum(ure * im - uim * re, axis=1, keepdims=True)
        inverse = 1.0 / square
        pre = pre * inverse
        pim = pim * inverse
        unit = 1.0 / jnp.sqrt(square)
        re, im = (
            jnp.where(rows > k, re - pre * ure + pim * uim, jnp.where(rows == k, ure * unit, re)),
            jnp.where(rows > k, im - pre * uim - pim * ure, jnp.where(rows == k, uim * unit, im)),
        )
    return (re, im)


def solve_kernel(total, parts, counts, out):
    count, half, _ = parts.shape
    summed = parts[0].astype(F32)
    for index in range(1, count):
        summed = summed + parts[index].astype(F32)
    summed = summed / total
    flipped = summed.T
    rows, cols = iotas((half, half))
    gram_re = jnp.where(cols >= rows, summed, flipped)
    gram_im = jnp.where(cols < rows, summed, jnp.where(cols > rows, -flipped, 0.0))
    operator = jnp.concatenate(
        [
            jnp.concatenate([gram_re, -gram_im], axis=1),
            jnp.concatenate([gram_im, gram_re], axis=1),
        ],
        axis=0,
    )
    high = operator.astype(BF16)
    low = (operator - high.astype(F32)).astype(BF16)

    def apply(re, im):
        vectors = jnp.concatenate([re, im], axis=1)
        vhigh = vectors.astype(BF16)
        vlow = (vectors - vhigh.astype(F32)).astype(BF16)
        both = jnp.concatenate([vhigh, vlow], axis=0)
        first = jnp.dot(both, high, preferred_element_type=F32)
        second = jnp.dot(both, low, preferred_element_type=F32)
        image = first[:KMAX] + first[KMAX:] + second[:KMAX]
        return (image[:, :half], image[:, half:])

    re, im = orthonormal(gram_re[:KMAX], -gram_im[:KMAX])
    for _ in range(ITERS - 1):
        re, im = orthonormal(*apply(re, im))
    image_re, image_im = apply(re, im)
    energy = jnp.sum(re * image_re + im * image_im, axis=1, keepdims=True)
    kept = counts[lax.axis_index("space")]
    ranks, lanes = iotas((KMAX, half))
    scale = jnp.where(ranks[:, :1] < kept, 1.0 / jnp.sqrt(energy + EPS), 0.0)
    first = energy.astype(BF16)
    rest = energy - first.astype(F32)
    second = rest.astype(BF16)
    third = (rest - second.astype(F32)).astype(BF16)
    tail = jnp.where(
        lanes == 0,
        first.astype(F32),
        jnp.where(lanes == 1, second.astype(F32), jnp.where(lanes == 2, third.astype(F32), 0.0)),
    )
    message = jnp.concatenate([re * scale, im * scale, tail], axis=1).astype(BF16)
    for index in range(out.shape[0]):
        out[index] = message


def solve(parts, counts, total):
    _, half, _ = parts.shape
    return pl.pallas_call(
        functools.partial(solve_kernel, total),
        in_specs=[VMEM, SMEM],
        out_specs=VMEM,
        out_shape=jax.ShapeDtypeStruct((counts.shape[0], KMAX, 3 * half), BF16),
        compiler_params=kernel_params(8),
        cost_estimate=cost(8_000_000_000, parts.size * 2),
        name="solve",
    )(parts, counts)


def coefficient_rows(message, half):
    part_re = message[:, :half]
    part_im = message[:, half : 2 * half]
    return jnp.concatenate(
        [
            jnp.concatenate([part_re, -part_im], axis=1),
            jnp.concatenate([part_im, part_re], axis=1),
        ],
        axis=0,
    )


def project(rows, block):
    return lax.dot_general(
        rows, block, (((1,), (1,)), ((), ())), preferred_element_type=F32
    ).astype(BF16)


def part_kernel(begin, size, messages, partner, resident, *rest):
    out = rest[-1]
    groups, points, width = resident.shape
    start = pl.multiple_of((1 - kept_half()) * (points // 2) + begin, 128)
    for index in range(groups):
        rows = coefficient_rows(messages[index], width // 2)
        out[index] = project(rows, resident[index, pl.ds(start, size)])
    if out.shape[0] > groups:
        _, lanes = iotas((2 * KMAX, size))
        table = jnp.zeros((2 * KMAX, size), jnp.int32)
        for index in range(groups):
            table = jnp.where(lanes // (2 * KMAX) == index, partner[index], table)
        out[groups] = table.astype(F32).astype(BF16)


def modes_part(messages, partner, resident, begin, size, *after):
    groups, _, width = resident.shape
    planes = groups if after else groups + 1
    return pl.pallas_call(
        functools.partial(part_kernel, begin, size),
        in_specs=[VMEM, SMEM, VMEM] + [ANY] * len(after),
        out_specs=VMEM,
        out_shape=jax.ShapeDtypeStruct((planes, 2 * KMAX, size), BF16),
        compiler_params=kernel_params(8),
        cost_estimate=cost(2_000_000_000, groups * size * width * 2),
        name="modes_part",
    )(messages, partner, resident, *after)


def modes_kernel(slots, messages, weight, resident, after, out, energy, high, low, made, put):
    groups, points, width = resident.shape
    part = points // 2
    start = pl.multiple_of(kept_half() * part, 128)

    def store(step, slot):
        return pltpu.make_async_copy(made.at[slot], out.at[step], put.at[slot])

    _, lanes = iotas(energy.shape)
    value = jnp.zeros(energy.shape, F32)
    for index in range(groups):
        column = jnp.sum(messages[index, :, width:].astype(F32), axis=1, keepdims=True)
        value = jnp.where(lanes == index, column, value)
    energy[...] = value

    def body(step, carry):
        slot = lax.rem(step, slots)

        @pl.when(step >= slots)
        def _():
            store(step - slots, slot).wait()

        made[slot] = project(coefficient_rows(messages[step], width // 2), resident[step])
        store(step, slot).start()
        own = made[slot, :, pl.ds(start, part)].astype(F32) * weight[:, pl.ds(start, part)]
        top = own.astype(BF16)
        high[step] = top
        low[step] = (own - top.astype(F32)).astype(BF16)
        return carry

    lax.fori_loop(0, groups, body, 0)
    for slot in range(slots):
        store(groups - slots + slot, slot).wait()


def modes_all(messages, weight, resident, after):
    groups, points, width = resident.shape
    slots = 4
    weighted = jax.ShapeDtypeStruct((groups, 2 * KMAX, points // 2), BF16)
    return pl.pallas_call(
        functools.partial(modes_kernel, slots),
        in_specs=[VMEM, VMEM, VMEM, ANY],
        out_specs=(HBM, VMEM, VMEM, VMEM),
        out_shape=(
            jax.ShapeDtypeStruct((groups, 2 * KMAX, points), BF16),
            jax.ShapeDtypeStruct((KMAX, groups), F32),
            weighted,
            weighted,
        ),
        scratch_shapes=[
            pltpu.VMEM((slots, 2 * KMAX, points), BF16),
            pltpu.SemaphoreType.DMA((slots,)),
        ],
        compiler_params=kernel_params(12),
        cost_estimate=cost(7_000_000_000, groups * points * width * 2),
        name="modes_all",
    )(messages, weight, resident, after)


def lane_table(partner, rank):
    groups = partner.shape[0]
    _, lanes = iotas((KMAX, groups * rank))
    table = jnp.zeros((KMAX, groups * rank), jnp.int32)
    for index in range(groups):
        table = jnp.where(lanes // rank == index, partner[index], table)
    return table


def chosen(cross, lane_partner, groups):
    rank = 2 * KMAX
    top = jnp.zeros((KMAX, groups * rank), F32)
    bottom = jnp.zeros((KMAX, groups * rank), F32)
    for index in range(groups):
        taken = lane_partner == index
        top = jnp.where(taken, cross[index * rank : index * rank + KMAX], top)
        bottom = jnp.where(taken, cross[index * rank + KMAX : (index + 1) * rank], bottom)
    _, lanes = iotas(top.shape)
    width = groups * rank
    return jnp.where(
        lanes % rank < KMAX,
        top + pltpu.roll(bottom, width - KMAX, 1),
        pltpu.roll(bottom, KMAX, 1) - top,
    )


def cross_kernel(own_partner, high, low, *rest):
    arrived, out = (rest[:-1], rest[-1])
    groups, rank, part = high.shape
    rows = groups * rank
    cross = jnp.zeros((rows, rows), F32)
    begin = 0
    for share in arrived:
        size = share.shape[2]
        other = share[:groups].reshape(rows, size)
        for own in (high, low):
            mine = own[:, :, begin : begin + size].reshape(rows, size)
            cross = cross + lax.dot_general(
                mine, other, (((1,), (1,)), ((), ())), preferred_element_type=F32
            )
        begin += size
    other_table = arrived[0][groups, :KMAX, :rows].astype(F32).astype(jnp.int32)
    own_value = chosen(cross.T, lane_table(own_partner, rank), groups)
    other_value = chosen(cross, other_table, groups)
    both = jnp.concatenate([own_value, other_value], axis=0).astype(BF16)
    source, target = iotas((rows, rows))
    moved = target == (source % rank) * groups + source // rank
    ordered = jnp.dot(both, moved.astype(F32).astype(BF16), preferred_element_type=F32)
    first = kept_half() == 0
    lower = jnp.where(first, ordered[:KMAX], ordered[KMAX:]).astype(BF16)
    upper = jnp.where(first, ordered[KMAX:], ordered[:KMAX]).astype(BF16)
    half = out.shape[0] // 2
    for index in range(half):
        out[index] = lower
        out[half + index] = upper


def cross_sums(own_partner, high, low, arrived, members):
    groups, rank, part = high.shape
    return pl.pallas_call(
        cross_kernel,
        in_specs=[SMEM] + [VMEM] * (2 + len(arrived)),
        out_specs=VMEM,
        out_shape=jax.ShapeDtypeStruct((members, KMAX, groups * rank), BF16),
        compiler_params=kernel_params(16),
        cost_estimate=cost(2_000_000_000, 4 * high.size),
        name="cross_sums",
    )(own_partner, high, low, *arrived)


def finish_kernel(total, parts, out):
    summed = parts[0].astype(F32)
    for index in range(1, parts.shape[0]):
        summed = summed + parts[index].astype(F32)
    summed = summed / total
    groups = out.shape[3]
    for side in range(2):
        for k in range(KMAX):
            begin = (side * KMAX + k) * groups
            out[side, k] = summed[:, begin : begin + groups]


def finish(parts, total):
    _, kmax, width = parts.shape
    return pl.pallas_call(
        functools.partial(finish_kernel, total),
        in_specs=[VMEM],
        out_specs=VMEM,
        out_shape=jax.ShapeDtypeStruct((2, kmax, kmax, width // (2 * kmax)), F32),
        compiler_params=kernel_params(8),
        cost_estimate=cost(1_000_000, parts.size * 2),
        name="finish",
    )(parts)


def on_device(spectra, weight, partner, counts):
    groups, points, width = spectra.shape
    n_freq, n_space = (lax.axis_size("freq"), lax.axis_size("space"))
    total = points * n_space
    spectra = pltpu.with_memory_space_constraint(spectra, pltpu.HBM)
    weight_row = weight[None, :]
    mirror = [(index, n_freq - 1 - index) for index in range(n_freq)]

    mine, other, resident = gram(
        spectra, pltpu.with_memory_space_constraint(weight_row, pltpu.HBM)
    )
    resident = pltpu.with_memory_space_constraint(resident, pltpu.VMEM)
    swapped = lax.ppermute(other, "space", [(index, index ^ 1) for index in range(n_space)])
    chips = [[index for index in range(core, n_space, 2)] for core in range(2)]
    parts = lax.all_to_all(
        (mine + swapped).astype(BF16), "space", 0, 0, tiled=True, axis_index_groups=chips
    )
    message = solve(parts, counts, total)
    messages = lax.all_to_all(message, "space", 0, 0, tiled=True)

    part = points // 2
    cut = part // 3
    first_share = modes_part(messages, partner, resident, 0, cut)
    shares = [
        first_share,
        modes_part(messages, partner, resident, cut, part - cut, first_share),
    ]
    arrived = [lax.ppermute(share, "freq", mirror) for share in shares]
    modes, energy, high, low = modes_all(messages, weight_row, resident, shares[-1])

    members = [
        [group * n_space + index for group in (low_group, n_freq - 1 - low_group) for index in range(n_space)]
        for low_group in range(n_freq // 2)
    ]
    gathered = lax.all_to_all(
        cross_sums(partner, high, low, arrived, 2 * n_space),
        ("freq", "space"),
        0,
        0,
        tiled=True,
        axis_index_groups=members,
    )
    coherence = jnp.transpose(finish(gathered, total), (3, 0, 1, 2))
    return (modes, jnp.transpose(energy), coherence)


def solution(mesh):
    in_specs = (P("freq", "space", None), P("space"), P("freq"), P("freq"))
    out_specs = (P("freq", None, "space"), P("freq", None), P("freq", None, None, None))
    return jax.shard_map(
        on_device, mesh=mesh, in_specs=in_specs, out_specs=out_specs, check_vma=False
    )
```

```python
import functools

import jax
import jax.numpy as jnp
from jax import lax
from jax.experimental import pallas as pl
from jax.experimental.pallas import tpu as pltpu
from jax.sharding import PartitionSpec as P

KMAX = 8
ITERS = 4
EPS = 1e-06
F32 = jnp.float32
BF16 = jnp.bfloat16
VMEM = pl.BlockSpec(memory_space=pltpu.VMEM)
SMEM = pl.BlockSpec(memory_space=pltpu.SMEM)
ANY = pl.BlockSpec(memory_space=pl.ANY)
HBM = pl.BlockSpec(memory_space=pltpu.HBM)


def kernel_params(mebibytes):
    return pltpu.CompilerParams(vmem_limit_bytes=mebibytes * 1024 * 1024)


def cost(flops, moved):
    return pl.CostEstimate(flops=flops, bytes_accessed=moved, transcendentals=0)


def kept_half():
    return jnp.where(lax.axis_index("freq") < lax.axis_size("freq") // 2, 0, 1)


def iotas(shape):
    return (
        lax.broadcasted_iota(jnp.int32, shape, 0),
        lax.broadcasted_iota(jnp.int32, shape, 1),
    )


def gram_kernel(depth, per_step, spectra, weight, mine, other, resident, scale, sems, scale_sem):
    groups, points, width = spectra.shape
    half = width // 2
    steps = groups // per_step
    rows, cols = iotas((half, half))
    south = lax.rem(lax.axis_index("space"), 2) == 0

    def fetch(step):
        part = pl.ds(step * per_step, per_step)
        return pltpu.make_async_copy(spectra.at[part], resident.at[part], sems.at[step])

    fetch(0).start()
    scale_copy = pltpu.make_async_copy(weight, scale, scale_sem)
    scale_copy.start()
    for step in range(1, depth):
        fetch(step).start()
    scale_copy.wait()

    def hermitian(index):
        block = resident[index]
        weighted = (block.T.astype(F32) * scale[...]).astype(BF16)
        moment = jnp.dot(weighted, block, preferred_element_type=F32)
        real = moment[:half, :half] + moment[half:, half:]
        imag = moment[:half, half:] - moment[half:, :half]
        return jnp.where(cols >= rows, real, imag)

    def body(step, carry):
        fetch(step).wait()

        @pl.when(step + depth < steps)
        def _():
            fetch(step + depth).start()

        for index in range(0, per_step, 2):
            even = hermitian(step * per_step + index)
            odd = hermitian(step * per_step + index + 1)
            place = (step * per_step + index) // 2
            mine[place] = jnp.where(south, even, odd)
            other[place] = jnp.where(south, odd, even)
        return carry

    lax.fori_loop(0, steps, body, 0)


def gram(spectra, weight):
    groups, points, width = spectra.shape
    half = width // 2
    depth, per_step = (2, 2)
    sums = jax.ShapeDtypeStruct((groups // 2, half, half), F32)
    return pl.pallas_call(
        functools.partial(gram_kernel, depth, per_step),
        in_specs=[HBM, HBM],
        out_specs=(VMEM, VMEM, VMEM),
        out_shape=(sums, sums, pltpu.VMEM((groups, points, width), BF16)),
        scratch_shapes=[
            pltpu.VMEM((1, points), F32),
            pltpu.SemaphoreType.DMA((groups // per_step,)),
            pltpu.SemaphoreType.DMA,
        ],
        compiler_params=kernel_params(16),
        cost_estimate=cost(2 * groups * points * width * width, groups * points * width * 2),
        name="gram",
    )(spectra, weight)


def orthonormal(re, im):
    rows, _ = iotas(re.shape)
    for k in range(KMAX):
        ure = jnp.broadcast_to(re[k : k + 1], re.shape)
        uim = jnp.broadcast_to(im[k : k + 1], im.shape)
        square = jnp.sum(ure * ure + uim * uim, axis=1, keepdims=True) + EPS
        pre = jnp.sum(ure * re + uim * im, axis=1, keepdims=True)
        pim = jnp.sum(ure * im - uim * re, axis=1, keepdims=True)
        unit = lax.rsqrt(square)
        inverse = unit * unit
        pre = pre * inverse
        pim = pim * inverse
        re, im = (
            jnp.where(rows > k, re - pre * ure + pim * uim, jnp.where(rows == k, ure * unit, re)),
            jnp.where(rows > k, im - pre * uim - pim * ure, jnp.where(rows == k, uim * unit, im)),
        )
    return (re, im)


def solve_kernel(total, parts, counts, partner, out, table, kept_all, partners, sems):
    count, half, _ = parts.shape
    small = (
        pltpu.make_async_copy(counts, kept_all, sems.at[0]),
        pltpu.make_async_copy(partner, partners, sems.at[1]),
    )
    for copy in small:
        copy.start()
    summed = parts[0].astype(F32)
    for index in range(1, count):
        summed = summed + parts[index].astype(F32)
    summed = summed / total
    flipped = summed.T
    rows, cols = iotas((half, half))
    gram_re = jnp.where(cols >= rows, summed, flipped)
    gram_im = jnp.where(cols < rows, summed, jnp.where(cols > rows, -flipped, 0.0))
    operator = jnp.concatenate(
        [
            jnp.concatenate([gram_re, -gram_im], axis=1),
            jnp.concatenate([gram_im, gram_re], axis=1),
        ],
        axis=0,
    )
    high = operator.astype(BF16)
    low = (operator - high.astype(F32)).astype(BF16)

    def apply(re, im):
        vectors = jnp.concatenate([re, im], axis=1)
        vhigh = vectors.astype(BF16)
        vlow = (vectors - vhigh.astype(F32)).astype(BF16)
        both = jnp.concatenate([vhigh, vlow], axis=0)
        first = jnp.dot(both, high, preferred_element_type=F32)
        second = jnp.dot(both, low, preferred_element_type=F32)
        image = first[:KMAX] + first[KMAX:] + second[:KMAX]
        return (image[:, :half], image[:, half:])

    re, im = orthonormal(gram_re[:KMAX], -gram_im[:KMAX])
    for _ in range(ITERS - 1):
        re, im = orthonormal(*apply(re, im))
    image_re, image_im = apply(re, im)
    energy = jnp.sum(re * image_re + im * image_im, axis=1, keepdims=True)
    for copy in small:
        copy.wait()
    kept = kept_all[lax.axis_index("space")]
    ranks, lanes = iotas((KMAX, half))
    scale = jnp.where(ranks[:, :1] < kept, 1.0 / jnp.sqrt(energy + EPS), 0.0)
    first = energy.astype(BF16)
    rest = energy - first.astype(F32)
    second = rest.astype(BF16)
    third = (rest - second.astype(F32)).astype(BF16)
    tail = jnp.where(
        lanes == 0,
        first.astype(F32),
        jnp.where(lanes == 1, second.astype(F32), jnp.where(lanes == 2, third.astype(F32), 0.0)),
    )
    message = jnp.concatenate([re * scale, im * scale, tail], axis=1).astype(BF16)
    for index in range(out.shape[0]):
        out[index] = message
    _, lanes = iotas(table.shape)
    value = jnp.zeros(table.shape, jnp.int32)
    for index in range(partners.shape[0]):
        value = jnp.where(lanes // (2 * KMAX) == index, partners[index], value)
    table[...] = value.astype(F32).astype(BF16)


def solve(parts, counts, partner, total, lanes):
    _, half, _ = parts.shape
    groups = counts.shape[0]
    return pl.pallas_call(
        functools.partial(solve_kernel, total),
        in_specs=[VMEM, HBM, HBM],
        out_specs=(VMEM, VMEM),
        out_shape=(
            jax.ShapeDtypeStruct((groups, KMAX, 3 * half), BF16),
            jax.ShapeDtypeStruct((2 * KMAX, lanes), BF16),
        ),
        scratch_shapes=[
            pltpu.SMEM((groups,), jnp.int32),
            pltpu.SMEM((groups,), jnp.int32),
            pltpu.SemaphoreType.DMA((2,)),
        ],
        compiler_params=kernel_params(8),
        cost_estimate=cost(8_000_000_000, parts.size * 2),
        name="solve",
    )(parts, counts, partner)


def coefficient_rows(message, half):
    part_re = message[:, :half]
    part_im = message[:, half : 2 * half]
    return jnp.concatenate(
        [
            jnp.concatenate([part_re, -part_im], axis=1),
            jnp.concatenate([part_im, part_re], axis=1),
        ],
        axis=0,
    )


def project(rows, block):
    return lax.dot_general(
        rows, block, (((1,), (1,)), ((), ())), preferred_element_type=F32
    ).astype(BF16)


def part_kernel(begin, size, messages, table, resident, *rest):
    out = rest[-1]
    groups, points, width = resident.shape
    start = pl.multiple_of((1 - kept_half()) * (points // 2) + begin, 128)
    for index in range(groups):
        rows = coefficient_rows(messages[index], width // 2)
        out[index] = project(rows, resident[index, pl.ds(start, size)])
    if out.shape[0] > groups:
        out[groups] = table[...]


def modes_part(messages, table, resident, begin, size, planes, *after):
    groups, _, width = resident.shape
    return pl.pallas_call(
        functools.partial(part_kernel, begin, size),
        in_specs=[VMEM, VMEM, VMEM] + [ANY] * len(after),
        out_specs=VMEM,
        out_shape=jax.ShapeDtypeStruct((planes, 2 * KMAX, size), BF16),
        compiler_params=kernel_params(8),
        cost_estimate=cost(2_000_000_000, groups * size * width * 2),
        name="modes_part",
    )(messages, table, resident, *after)


def modes_kernel(slots, per_turn, messages, weight, resident, after, out, energy, high, low, made, put):
    groups, points, width = resident.shape
    part = points // 2
    upper = kept_half() == 1
    scale = weight[:, pl.ds(pl.multiple_of(kept_half() * part, 128), part)]

    def store(step, slot):
        return pltpu.make_async_copy(made.at[slot], out.at[step], put.at[slot])

    _, lanes = iotas(energy.shape)
    value = jnp.zeros(energy.shape, F32)
    for index in range(groups):
        column = jnp.sum(messages[index, :, width:].astype(F32), axis=1, keepdims=True)
        value = jnp.where(lanes == index, column, value)
    energy[...] = value

    def body(turn, carry):
        for offset in range(per_turn):
            step = turn * per_turn + offset
            slot = lax.rem(step, slots)

            @pl.when(step >= slots)
            def _():
                store(step - slots, slot).wait()

        for offset in range(per_turn):
            step = turn * per_turn + offset
            slot = lax.rem(step, slots)
            value = project(coefficient_rows(messages[step], width // 2), resident[step])
            made[slot] = value
            own = jnp.where(upper, value[:, part:], value[:, :part]).astype(F32) * scale
            top = own.astype(BF16)
            high[step] = top
            low[step] = (own - top.astype(F32)).astype(BF16)
        for offset in range(per_turn):
            step = turn * per_turn + offset
            store(step, lax.rem(step, slots)).start()
        return carry

    lax.fori_loop(0, groups // per_turn, body, 0)
    for slot in range(slots):
        store(groups - slots + slot, slot).wait()


def modes_all(messages, weight, resident, after):
    groups, points, width = resident.shape
    slots = 4
    weighted = jax.ShapeDtypeStruct((groups, 2 * KMAX, points // 2), BF16)
    return pl.pallas_call(
        functools.partial(modes_kernel, slots, 2),
        in_specs=[VMEM, VMEM, VMEM, ANY],
        out_specs=(HBM, VMEM, VMEM, VMEM),
        out_shape=(
            jax.ShapeDtypeStruct((groups, 2 * KMAX, points), BF16),
            jax.ShapeDtypeStruct((KMAX, groups), F32),
            weighted,
            weighted,
        ),
        scratch_shapes=[
            pltpu.VMEM((slots, 2 * KMAX, points), BF16),
            pltpu.SemaphoreType.DMA((slots,)),
        ],
        compiler_params=kernel_params(12),
        cost_estimate=cost(7_000_000_000, groups * points * width * 2),
        name="modes_all",
    )(messages, weight, resident, after)


def chosen(cross, lane_partner, groups):
    rank = 2 * KMAX
    top = jnp.zeros((KMAX, groups * rank), F32)
    bottom = jnp.zeros((KMAX, groups * rank), F32)
    for index in range(groups):
        taken = lane_partner == index
        top = jnp.where(taken, cross[index * rank : index * rank + KMAX], top)
        bottom = jnp.where(taken, cross[index * rank + KMAX : (index + 1) * rank], bottom)
    _, lanes = iotas(top.shape)
    width = groups * rank
    return jnp.where(
        lanes % rank < KMAX,
        top + pltpu.roll(bottom, width - KMAX, 1),
        pltpu.roll(bottom, KMAX, 1) - top,
    )


def products(high, low, share, begin):
    groups, rank, _ = high.shape
    rows, size = (groups * rank, share.shape[2])
    other = share[:groups].reshape(rows, size)
    total = None
    for own in (high, low):
        mine = own[:, :, begin : begin + size].reshape(rows, size)
        part = lax.dot_general(mine, other, (((1,), (1,)), ((), ())), preferred_element_type=F32)
        total = part if total is None else total + part
    return total


def early_kernel(begins, high, low, *rest):
    arrived, out = (rest[:-1], rest[-1])
    value = products(high, low, arrived[0], begins[0])
    for share, begin in zip(arrived[1:], begins[1:]):
        value = value + products(high, low, share, begin)
    out[...] = value


def early_products(high, low, arrived, begins):
    rows = high.shape[0] * high.shape[1]
    return pl.pallas_call(
        functools.partial(early_kernel, begins),
        in_specs=[VMEM] * (2 + len(arrived)),
        out_specs=VMEM,
        out_shape=jax.ShapeDtypeStruct((rows, rows), F32),
        compiler_params=kernel_params(8),
        cost_estimate=cost(2_000_000_000, 4 * high.size),
        name="early_products",
    )(high, low, *arrived)


def cross_kernel(begin, early, table, high, low, share, out):
    groups, rank, part = high.shape
    rows = groups * rank
    cross = early[...] + products(high, low, share, begin)
    own_table = table[:KMAX, :rows].astype(F32).astype(jnp.int32)
    other_table = share[groups, :KMAX, :rows].astype(F32).astype(jnp.int32)
    own_value = chosen(cross.T, own_table, groups)
    other_value = chosen(cross, other_table, groups)
    both = jnp.concatenate([own_value, other_value], axis=0).astype(BF16)
    source, target = iotas((rows, rows))
    moved = target == (source % rank) * groups + source // rank
    ordered = jnp.dot(both, moved.astype(F32).astype(BF16), preferred_element_type=F32)
    first = kept_half() == 0
    lower = jnp.where(first, ordered[:KMAX], ordered[KMAX:]).astype(BF16)
    upper = jnp.where(first, ordered[KMAX:], ordered[:KMAX]).astype(BF16)
    half = out.shape[0] // 2
    for index in range(half):
        out[index] = lower
        out[half + index] = upper


def cross_sums(early, table, high, low, share, begin, members):
    groups, rank, part = high.shape
    return pl.pallas_call(
        functools.partial(cross_kernel, begin),
        in_specs=[VMEM] * 5,
        out_specs=VMEM,
        out_shape=jax.ShapeDtypeStruct((members, KMAX, groups * rank), BF16),
        compiler_params=kernel_params(8),
        cost_estimate=cost(2_000_000_000, 4 * high.size),
        name="cross_sums",
    )(early, table, high, low, share)


def finish_kernel(total, parts, out):
    summed = parts[0].astype(F32)
    for index in range(1, parts.shape[0]):
        summed = summed + parts[index].astype(F32)
    summed = summed / total
    groups = out.shape[3]
    for side in range(2):
        for k in range(KMAX):
            begin = (side * KMAX + k) * groups
            out[side, k] = summed[:, begin : begin + groups]


def finish(parts, total):
    _, kmax, width = parts.shape
    return pl.pallas_call(
        functools.partial(finish_kernel, total),
        in_specs=[VMEM],
        out_specs=VMEM,
        out_shape=jax.ShapeDtypeStruct((2, kmax, kmax, width // (2 * kmax)), F32),
        compiler_params=kernel_params(8),
        cost_estimate=cost(1_000_000, parts.size * 2),
        name="finish",
    )(parts)


def on_device(spectra, weight, partner, counts):
    groups, points, width = spectra.shape
    n_freq, n_space = (lax.axis_size("freq"), lax.axis_size("space"))
    total = points * n_space
    spectra = pltpu.with_memory_space_constraint(spectra, pltpu.HBM)
    weight_row = weight[None, :]
    mirror = [(index, n_freq - 1 - index) for index in range(n_freq)]

    mine, other, resident = gram(
        spectra, pltpu.with_memory_space_constraint(weight_row, pltpu.HBM)
    )
    resident = pltpu.with_memory_space_constraint(resident, pltpu.VMEM)
    swapped = lax.ppermute(other, "space", [(index, index ^ 1) for index in range(n_space)])
    chips = [[index for index in range(core, n_space, 2)] for core in range(2)]
    parts = lax.all_to_all(
        (mine + swapped).astype(BF16), "space", 0, 0, tiled=True, axis_index_groups=chips
    )
    part = points // 2
    sizes = (part // 4, part // 2, part // 4)
    begins = (0, part // 4, 3 * part // 4)
    in_hbm = [pltpu.with_memory_space_constraint(array, pltpu.HBM) for array in (counts, partner)]
    message, table = solve(parts, *in_hbm, total, sizes[-1])
    messages = lax.all_to_all(message, "space", 0, 0, tiled=True)

    shares = []
    for begin, size in zip(begins, sizes):
        planes = groups + 1 if size + begin == part else groups
        shares.append(modes_part(messages, table, resident, begin, size, planes, *shares[-1:]))
    arrived = [lax.ppermute(share, "freq", mirror) for share in shares]
    modes, energy, high, low = modes_all(messages, weight_row, resident, shares[-1])
    early = early_products(high, low, arrived[:-1], begins[:-1])

    members = [
        [group * n_space + index for group in (low_group, n_freq - 1 - low_group) for index in range(n_space)]
        for low_group in range(n_freq // 2)
    ]
    gathered = lax.all_to_all(
        cross_sums(
            early, table, high, low, arrived[-1], begins[-1], 2 * n_space
        ),
        ("freq", "space"),
        0,
        0,
        tiled=True,
        axis_index_groups=members,
    )
    coherence = jnp.transpose(finish(gathered, total), (3, 0, 1, 2))
    return (modes, jnp.transpose(energy), coherence)


def solution(mesh):
    in_specs = (P("freq", "space", None), P("space"), P("freq"), P("freq"))
    out_specs = (P("freq", None, "space"), P("freq", None), P("freq", None, None, None))
    return jax.shard_map(
        on_device, mesh=mesh, in_specs=in_specs, out_specs=out_specs, check_vma=False
    )
```

```python
import functools

import jax
import jax.numpy as jnp
from jax import lax
from jax.experimental import pallas as pl
from jax.experimental.pallas import tpu as pltpu
from jax.sharding import PartitionSpec as P

KMAX = 8
ITERS = 4
EPS = 1e-06
F32 = jnp.float32
BF16 = jnp.bfloat16
VMEM = pl.BlockSpec(memory_space=pltpu.VMEM)
SMEM = pl.BlockSpec(memory_space=pltpu.SMEM)
ANY = pl.BlockSpec(memory_space=pl.ANY)
HBM = pl.BlockSpec(memory_space=pltpu.HBM)


def kernel_params(mebibytes):
    return pltpu.CompilerParams(vmem_limit_bytes=mebibytes * 1024 * 1024)


def cost(flops, moved):
    return pl.CostEstimate(flops=flops, bytes_accessed=moved, transcendentals=0)


def kept_half():
    return jnp.where(lax.axis_index("freq") < lax.axis_size("freq") // 2, 0, 1)


def iotas(shape):
    return (
        lax.broadcasted_iota(jnp.int32, shape, 0),
        lax.broadcasted_iota(jnp.int32, shape, 1),
    )


def hermitian(block, scale):
    half = block.shape[1] // 2
    rows, cols = iotas((half, half))
    weighted = (block.T.astype(F32) * scale).astype(BF16)
    moment = jnp.dot(weighted, block, preferred_element_type=F32)
    real = moment[:half, :half] + moment[half:, half:]
    imag = moment[:half, half:] - moment[half:, :half]
    return jnp.where(cols >= rows, real, imag)


def on_core():
    return lax.rem(lax.axis_index("space"), 2)


def pair_copy(spectra, held, sems, side, pair, slot):
    begin = side * (spectra.shape[0] // 2) + 2 * pair
    return pltpu.make_async_copy(
        spectra.at[pl.ds(begin, 2)], held.at[pl.ds(2 * slot, 2)], sems.at[slot]
    )


def gram_other_kernel(spectra, weight, sums, theirs, ahead, scale, sems, ahead_sems, scale_sem):
    pairs = theirs.shape[0] // 2
    early = ahead.shape[0] // 2
    copies = [pair_copy(spectra, theirs, sems, 1 - on_core(), p, p) for p in range(pairs)]
    copies += [pair_copy(spectra, ahead, ahead_sems, on_core(), p, p) for p in range(early)]
    due = {0: (2, 3), 1: (4,), 2: (5,)}
    copies[0].start()
    scale_copy = pltpu.make_async_copy(weight, scale, scale_sem)
    scale_copy.start()
    copies[1].start()
    scale_copy.wait()
    for pair in range(pairs):
        copies[pair].wait()
        for later in due.get(pair, ()):
            copies[later].start()
        for index in range(2 * pair, 2 * pair + 2):
            sums[index] = hermitian(theirs[index], scale[...])
    for copy in copies[pairs:]:
        copy.wait()


def gram_mine_kernel(ahead, spectra, weight, sums, rest, scale, sems, scale_sem):
    early, late = (ahead.shape[0] // 2, rest.shape[0] // 2)
    copies = [pair_copy(spectra, rest, sems, on_core(), early + p, p) for p in range(late)]
    for copy in copies:
        copy.start()
    scale_copy = pltpu.make_async_copy(weight, scale, scale_sem)
    scale_copy.start()
    scale_copy.wait()
    for index in range(2 * early):
        sums[index] = hermitian(ahead[index], scale[...])
    for pair in range(late):
        copies[pair].wait()
        for index in range(2 * pair, 2 * pair + 2):
            sums[2 * early + index] = hermitian(rest[index], scale[...])


def gram_other(spectra, weight):
    groups, points, width = spectra.shape
    half = width // 2
    return pl.pallas_call(
        gram_other_kernel,
        in_specs=[HBM, HBM],
        out_specs=(VMEM, VMEM, VMEM),
        out_shape=(
            jax.ShapeDtypeStruct((groups // 2, half, half), F32),
            pltpu.VMEM((groups // 2, points, width), BF16),
            pltpu.VMEM((groups // 4, points, width), BF16),
        ),
        scratch_shapes=[
            pltpu.VMEM((1, points), F32),
            pltpu.SemaphoreType.DMA((groups // 4,)),
            pltpu.SemaphoreType.DMA((groups // 8,)),
            pltpu.SemaphoreType.DMA,
        ],
        compiler_params=kernel_params(16),
        cost_estimate=cost(groups * points * width * width, groups * points * width),
        name="gram_other",
    )(spectra, weight)


def gram_mine(ahead, spectra, weight):
    groups, points, width = spectra.shape
    half = width // 2
    return pl.pallas_call(
        gram_mine_kernel,
        in_specs=[VMEM, HBM, HBM],
        out_specs=(VMEM, VMEM),
        out_shape=(
            jax.ShapeDtypeStruct((groups // 2, half, half), F32),
            pltpu.VMEM((groups // 4, points, width), BF16),
        ),
        scratch_shapes=[
            pltpu.VMEM((1, points), F32),
            pltpu.SemaphoreType.DMA((groups // 8,)),
            pltpu.SemaphoreType.DMA,
        ],
        compiler_params=kernel_params(16),
        cost_estimate=cost(groups * points * width * width, groups * points * width),
        name="gram_mine",
    )(ahead, spectra, weight)


def orthonormal(re, im):
    rows, _ = iotas(re.shape)
    for k in range(KMAX):
        ure = jnp.broadcast_to(re[k : k + 1], re.shape)
        uim = jnp.broadcast_to(im[k : k + 1], im.shape)
        square = jnp.sum(ure * ure + uim * uim, axis=1, keepdims=True) + EPS
        pre = jnp.sum(ure * re + uim * im, axis=1, keepdims=True)
        pim = jnp.sum(ure * im - uim * re, axis=1, keepdims=True)
        unit = lax.rsqrt(square)
        inverse = unit * unit
        pre = pre * inverse
        pim = pim * inverse
        re, im = (
            jnp.where(rows > k, re - pre * ure + pim * uim, jnp.where(rows == k, ure * unit, re)),
            jnp.where(rows > k, im - pre * uim - pim * ure, jnp.where(rows == k, uim * unit, im)),
        )
    return (re, im)


def solve_kernel(total, parts, counts, partner, out, table, kept_all, partners, sems):
    count, half, _ = parts.shape
    small = (
        pltpu.make_async_copy(counts, kept_all, sems.at[0]),
        pltpu.make_async_copy(partner, partners, sems.at[1]),
    )
    for copy in small:
        copy.start()
    summed = parts[0].astype(F32)
    for index in range(1, count):
        summed = summed + parts[index].astype(F32)
    summed = summed / total
    flipped = summed.T
    rows, cols = iotas((half, half))
    gram_re = jnp.where(cols >= rows, summed, flipped)
    gram_im = jnp.where(cols < rows, summed, jnp.where(cols > rows, -flipped, 0.0))
    operator = jnp.concatenate(
        [
            jnp.concatenate([gram_re, -gram_im], axis=1),
            jnp.concatenate([gram_im, gram_re], axis=1),
        ],
        axis=0,
    )
    high = operator.astype(BF16)
    low = (operator - high.astype(F32)).astype(BF16)

    def apply(re, im):
        vectors = jnp.concatenate([re, im], axis=1)
        vhigh = vectors.astype(BF16)
        vlow = (vectors - vhigh.astype(F32)).astype(BF16)
        both = jnp.concatenate([vhigh, vlow], axis=0)
        first = jnp.dot(both, high, preferred_element_type=F32)
        second = jnp.dot(both, low, preferred_element_type=F32)
        image = first[:KMAX] + first[KMAX:] + second[:KMAX]
        return (image[:, :half], image[:, half:])

    re, im = orthonormal(gram_re[:KMAX], -gram_im[:KMAX])
    for _ in range(ITERS - 1):
        re, im = orthonormal(*apply(re, im))
    image_re, image_im = apply(re, im)
    energy = jnp.sum(re * image_re + im * image_im, axis=1, keepdims=True)
    for copy in small:
        copy.wait()
    place = lax.axis_index("space")
    kept = kept_all[lax.rem(place, 2) * (kept_all.shape[0] // 2) + place // 2]
    ranks, lanes = iotas((KMAX, half))
    scale = jnp.where(ranks[:, :1] < kept, 1.0 / jnp.sqrt(energy + EPS), 0.0)
    first = energy.astype(BF16)
    rest = energy - first.astype(F32)
    second = rest.astype(BF16)
    third = (rest - second.astype(F32)).astype(BF16)
    tail = jnp.where(
        lanes == 0,
        first.astype(F32),
        jnp.where(lanes == 1, second.astype(F32), jnp.where(lanes == 2, third.astype(F32), 0.0)),
    )
    message = jnp.concatenate([re * scale, im * scale, tail], axis=1).astype(BF16)
    for index in range(out.shape[0]):
        out[index] = message
    _, lanes = iotas(table.shape)
    value = jnp.zeros(table.shape, jnp.int32)
    for index in range(partners.shape[0]):
        value = jnp.where(lanes // (2 * KMAX) == index, partners[index], value)
    table[...] = value.astype(F32).astype(BF16)


def solve(parts, counts, partner, total, lanes):
    _, half, _ = parts.shape
    groups = counts.shape[0]
    return pl.pallas_call(
        functools.partial(solve_kernel, total),
        in_specs=[VMEM, HBM, HBM],
        out_specs=(VMEM, VMEM),
        out_shape=(
            jax.ShapeDtypeStruct((groups, KMAX, 3 * half), BF16),
            jax.ShapeDtypeStruct((2 * KMAX, lanes), BF16),
        ),
        scratch_shapes=[
            pltpu.SMEM((groups,), jnp.int32),
            pltpu.SMEM((groups,), jnp.int32),
            pltpu.SemaphoreType.DMA((2,)),
        ],
        compiler_params=kernel_params(8),
        cost_estimate=cost(8_000_000_000, parts.size * 2),
        name="solve",
    )(parts, counts, partner)


def place_of(index, groups):
    return 2 * (index % (groups // 2)) + index // (groups // 2)


def held_parts(theirs, ahead, rest):
    core = on_core()
    return ((theirs, 1 - core, 0), (ahead, core, 0), (rest, core, ahead.shape[0]))


def coefficient_rows(message, half):
    part_re = message[:, :half]
    part_im = message[:, half : 2 * half]
    return jnp.concatenate(
        [
            jnp.concatenate([part_re, -part_im], axis=1),
            jnp.concatenate([part_im, part_re], axis=1),
        ],
        axis=0,
    )


def project(rows, block):
    return lax.dot_general(
        rows, block, (((1,), (1,)), ((), ())), preferred_element_type=F32
    ).astype(BF16)


def part_kernel(begin, size, messages, table, theirs, ahead, rest, *more):
    out = more[-1]
    groups = messages.shape[0]
    _, points, width = theirs.shape
    start = pl.multiple_of((1 - kept_half()) * (points // 2) + begin, 128)
    for held, side, first in held_parts(theirs, ahead, rest):
        for index in range(held.shape[0]):
            rows = coefficient_rows(messages[2 * (first + index) + side], width // 2)
            target = side * (groups // 2) + first + index
            out[target] = project(rows, held[index, pl.ds(start, size)])
    if out.shape[0] > groups:
        out[groups] = table[...]


def modes_part(messages, table, held, begin, size, planes, *after):
    groups = messages.shape[0]
    width = held[0].shape[2]
    return pl.pallas_call(
        functools.partial(part_kernel, begin, size),
        in_specs=[VMEM] * 5 + [ANY] * len(after),
        out_specs=VMEM,
        out_shape=jax.ShapeDtypeStruct((planes, 2 * KMAX, size), BF16),
        compiler_params=kernel_params(8),
        cost_estimate=cost(2_000_000_000, groups * size * width * 2),
        name="modes_part",
    )(messages, table, *held, *after)


def modes_kernel(slots, messages, weight, theirs, ahead, rest, after, out, energy, high, low, made, put):
    groups = messages.shape[0]
    _, points, width = theirs.shape
    part = points // 2
    upper = kept_half() == 1
    scale = weight[:, pl.ds(pl.multiple_of(kept_half() * part, 128), part)]
    _, lanes = iotas(energy.shape)
    value = jnp.zeros(energy.shape, F32)
    for index in range(groups):
        column = jnp.sum(
            messages[place_of(index, groups), :, width:].astype(F32), axis=1, keepdims=True
        )
        value = jnp.where(lanes == index, column, value)
    energy[...] = value

    def store(slot, target):
        return pltpu.make_async_copy(made.at[slot], out.at[target], put.at[slot])

    done = 0
    for held, side, first in held_parts(theirs, ahead, rest):

        def body(turn, carry, held=held, side=side, first=first, done=done):
            local = [2 * turn, 2 * turn + 1]
            places = [lax.rem(done + index, slots) for index in local]
            targets = [side * (groups // 2) + first + index for index in local]
            for index, slot, target in zip(local, places, targets):

                @pl.when(done + index >= slots)
                def _():
                    store(slot, target).wait()

            for index, slot, target in zip(local, places, targets):
                rows = coefficient_rows(messages[2 * (first + index) + side], width // 2)
                value = project(rows, held[index])
                made[slot] = value
                own = jnp.where(upper, value[:, part:], value[:, :part]).astype(F32) * scale
                top = own.astype(BF16)
                high[target] = top
                low[target] = (own - top.astype(F32)).astype(BF16)
            for slot, target in zip(places, targets):
                store(slot, target).start()
            return carry

        lax.fori_loop(0, held.shape[0] // 2, body, 0)
        done += held.shape[0]
    for slot in range(slots):
        store(slot, slot).wait()


def modes_all(messages, weight, held, after):
    groups = messages.shape[0]
    _, points, width = held[0].shape
    slots = 4
    weighted = jax.ShapeDtypeStruct((groups, 2 * KMAX, points // 2), BF16)
    return pl.pallas_call(
        functools.partial(modes_kernel, slots),
        in_specs=[VMEM] * 5 + [ANY],
        out_specs=(HBM, VMEM, VMEM, VMEM),
        out_shape=(
            jax.ShapeDtypeStruct((groups, 2 * KMAX, points), BF16),
            jax.ShapeDtypeStruct((KMAX, groups), F32),
            weighted,
            weighted,
        ),
        scratch_shapes=[
            pltpu.VMEM((slots, 2 * KMAX, points), BF16),
            pltpu.SemaphoreType.DMA((slots,)),
        ],
        compiler_params=kernel_params(12),
        cost_estimate=cost(7_000_000_000, groups * points * width * 2),
        name="modes_all",
    )(messages, weight, *held, after)


def chosen(cross, lane_partner, groups):
    rank = 2 * KMAX
    top = jnp.zeros((KMAX, groups * rank), F32)
    bottom = jnp.zeros((KMAX, groups * rank), F32)
    for index in range(groups):
        taken = lane_partner == index
        top = jnp.where(taken, cross[index * rank : index * rank + KMAX], top)
        bottom = jnp.where(taken, cross[index * rank + KMAX : (index + 1) * rank], bottom)
    _, lanes = iotas(top.shape)
    width = groups * rank
    return jnp.where(
        lanes % rank < KMAX,
        top + pltpu.roll(bottom, width - KMAX, 1),
        pltpu.roll(bottom, KMAX, 1) - top,
    )


def products(high, low, share, begin):
    groups, rank, _ = high.shape
    rows, size = (groups * rank, share.shape[2])
    other = share[:groups].reshape(rows, size)
    total = None
    for own in (high, low):
        mine = own[:, :, begin : begin + size].reshape(rows, size)
        part = lax.dot_general(mine, other, (((1,), (1,)), ((), ())), preferred_element_type=F32)
        total = part if total is None else total + part
    return total


def early_kernel(begins, high, low, *rest):
    arrived, out = (rest[:-1], rest[-1])
    value = products(high, low, arrived[0], begins[0])
    for share, begin in zip(arrived[1:], begins[1:]):
        value = value + products(high, low, share, begin)
    out[...] = value


def early_products(high, low, arrived, begins):
    rows = high.shape[0] * high.shape[1]
    return pl.pallas_call(
        functools.partial(early_kernel, begins),
        in_specs=[VMEM] * (2 + len(arrived)),
        out_specs=VMEM,
        out_shape=jax.ShapeDtypeStruct((rows, rows), F32),
        compiler_params=kernel_params(8),
        cost_estimate=cost(2_000_000_000, 4 * high.size),
        name="early_products",
    )(high, low, *arrived)


def cross_kernel(begin, early, table, high, low, share, out):
    groups, rank, part = high.shape
    rows = groups * rank
    cross = early[...] + products(high, low, share, begin)
    own_table = table[:KMAX, :rows].astype(F32).astype(jnp.int32)
    other_table = share[groups, :KMAX, :rows].astype(F32).astype(jnp.int32)
    own_value = chosen(cross.T, own_table, groups)
    other_value = chosen(cross, other_table, groups)
    both = jnp.concatenate([own_value, other_value], axis=0).astype(BF16)
    source, target = iotas((rows, rows))
    moved = target == (source % rank) * groups + source // rank
    ordered = jnp.dot(both, moved.astype(F32).astype(BF16), preferred_element_type=F32)
    first = kept_half() == 0
    lower = jnp.where(first, ordered[:KMAX], ordered[KMAX:]).astype(BF16)
    upper = jnp.where(first, ordered[KMAX:], ordered[:KMAX]).astype(BF16)
    half = out.shape[0] // 2
    for index in range(half):
        out[index] = lower
        out[half + index] = upper


def cross_sums(early, table, high, low, share, begin, members):
    groups, rank, part = high.shape
    return pl.pallas_call(
        functools.partial(cross_kernel, begin),
        in_specs=[VMEM] * 5,
        out_specs=VMEM,
        out_shape=jax.ShapeDtypeStruct((members, KMAX, groups * rank), BF16),
        compiler_params=kernel_params(8),
        cost_estimate=cost(2_000_000_000, 4 * high.size),
        name="cross_sums",
    )(early, table, high, low, share)


def finish_kernel(total, parts, out):
    summed = parts[0].astype(F32)
    for index in range(1, parts.shape[0]):
        summed = summed + parts[index].astype(F32)
    summed = summed / total
    groups = out.shape[3]
    for side in range(2):
        for k in range(KMAX):
            begin = (side * KMAX + k) * groups
            out[side, k] = summed[:, begin : begin + groups]


def finish(parts, total):
    _, kmax, width = parts.shape
    return pl.pallas_call(
        functools.partial(finish_kernel, total),
        in_specs=[VMEM],
        out_specs=VMEM,
        out_shape=jax.ShapeDtypeStruct((2, kmax, kmax, width // (2 * kmax)), F32),
        compiler_params=kernel_params(8),
        cost_estimate=cost(1_000_000, parts.size * 2),
        name="finish",
    )(parts)


def on_device(spectra, weight, partner, counts):
    groups, points, width = spectra.shape
    n_freq, n_space = (lax.axis_size("freq"), lax.axis_size("space"))
    total = points * n_space
    spectra = pltpu.with_memory_space_constraint(spectra, pltpu.HBM)
    weight_row = weight[None, :]
    mirror = [(index, n_freq - 1 - index) for index in range(n_freq)]

    weight_hbm = pltpu.with_memory_space_constraint(weight_row, pltpu.HBM)
    other, theirs, ahead = gram_other(spectra, weight_hbm)
    swapped = lax.ppermute(other, "space", [(index, index ^ 1) for index in range(n_space)])
    ahead = pltpu.with_memory_space_constraint(ahead, pltpu.VMEM)
    mine, rest = gram_mine(ahead, spectra, weight_hbm)
    held = [
        pltpu.with_memory_space_constraint(theirs, pltpu.VMEM),
        ahead,
        pltpu.with_memory_space_constraint(rest, pltpu.VMEM),
    ]
    chips = [[index for index in range(core, n_space, 2)] for core in range(2)]
    parts = lax.all_to_all(
        (mine + swapped).astype(BF16), "space", 0, 0, tiled=True, axis_index_groups=chips
    )
    part = points // 2
    sizes = (part // 4, part // 2, part // 4)
    begins = (0, part // 4, 3 * part // 4)
    in_hbm = [pltpu.with_memory_space_constraint(array, pltpu.HBM) for array in (counts, partner)]
    message, table = solve(parts, *in_hbm, total, sizes[-1])
    messages = lax.all_to_all(message, "space", 0, 0, tiled=True)

    shares = []
    for begin, size in zip(begins, sizes):
        planes = groups + 1 if size + begin == part else groups
        shares.append(modes_part(messages, table, held, begin, size, planes, *shares[-1:]))
    arrived = [lax.ppermute(share, "freq", mirror) for share in shares]
    modes, energy, high, low = modes_all(messages, weight_row, held, shares[-1])
    early = early_products(high, low, arrived[:-1], begins[:-1])

    members = [
        [group * n_space + index for group in (low_group, n_freq - 1 - low_group) for index in range(n_space)]
        for low_group in range(n_freq // 2)
    ]
    gathered = lax.all_to_all(
        cross_sums(
            early, table, high, low, arrived[-1], begins[-1], 2 * n_space
        ),
        ("freq", "space"),
        0,
        0,
        tiled=True,
        axis_index_groups=members,
    )
    coherence = jnp.transpose(finish(gathered, total), (3, 0, 1, 2))
    return (modes, jnp.transpose(energy), coherence)


def solution(mesh):
    in_specs = (P("freq", "space", None), P("space"), P("freq"), P("freq"))
    out_specs = (P("freq", None, "space"), P("freq", None), P("freq", None, None, None))
    return jax.shard_map(
        on_device, mesh=mesh, in_specs=in_specs, out_specs=out_specs, check_vma=False
    )
```

```python
import functools

import jax
import jax.numpy as jnp
from jax import lax
from jax.experimental import pallas as pl
from jax.experimental.pallas import tpu as pltpu
from jax.sharding import PartitionSpec as P

KMAX = 8
ITERS = 4
EPS = 1e-06
F32 = jnp.float32
BF16 = jnp.bfloat16
VMEM = pl.BlockSpec(memory_space=pltpu.VMEM)
SMEM = pl.BlockSpec(memory_space=pltpu.SMEM)
ANY = pl.BlockSpec(memory_space=pl.ANY)
HBM = pl.BlockSpec(memory_space=pltpu.HBM)


def kernel_params(mebibytes):
    return pltpu.CompilerParams(vmem_limit_bytes=mebibytes * 1024 * 1024)


def cost(flops, moved):
    return pl.CostEstimate(flops=flops, bytes_accessed=moved, transcendentals=0)


def kept_half():
    return jnp.where(lax.axis_index("freq") < lax.axis_size("freq") // 2, 0, 1)


def iotas(shape):
    return (
        lax.broadcasted_iota(jnp.int32, shape, 0),
        lax.broadcasted_iota(jnp.int32, shape, 1),
    )


def hermitian(block, scale):
    half = block.shape[1] // 2
    rows, cols = iotas((half, half))
    weighted = (block.T.astype(F32) * scale).astype(BF16)
    moment = jnp.dot(weighted, block, preferred_element_type=F32)
    real = moment[:half, :half] + moment[half:, half:]
    imag = moment[:half, half:] - moment[half:, :half]
    return jnp.where(cols >= rows, real, imag)


def on_core():
    return lax.rem(lax.axis_index("space"), 2)


def pair_copy(spectra, held, sems, side, pair, slot):
    begin = side * (spectra.shape[0] // 2) + 2 * pair
    return pltpu.make_async_copy(
        spectra.at[pl.ds(begin, 2)], held.at[pl.ds(2 * slot, 2)], sems.at[slot]
    )


def gram_other_kernel(spectra, weight, sums, theirs, ahead, scale, sems, ahead_sems, scale_sem):
    pairs = theirs.shape[0] // 2
    early = ahead.shape[0] // 2
    copies = [pair_copy(spectra, theirs, sems, 1 - on_core(), p, p) for p in range(pairs)]
    copies += [pair_copy(spectra, ahead, ahead_sems, on_core(), p, p) for p in range(early)]
    due = {0: (2, 3), 1: (4,), 2: (5,)}
    copies[0].start()
    scale_copy = pltpu.make_async_copy(weight, scale, scale_sem)
    scale_copy.start()
    copies[1].start()
    scale_copy.wait()
    for pair in range(pairs):
        copies[pair].wait()
        for later in due.get(pair, ()):
            copies[later].start()
        for index in range(2 * pair, 2 * pair + 2):
            sums[index] = hermitian(theirs[index], scale[...])
    for copy in copies[pairs:]:
        copy.wait()


def gram_mine_kernel(ahead, spectra, weight, sums, rest, scale, sems, scale_sem):
    early, late = (ahead.shape[0] // 2, rest.shape[0] // 2)
    copies = [pair_copy(spectra, rest, sems, on_core(), early + p, p) for p in range(late)]
    for copy in copies:
        copy.start()
    scale_copy = pltpu.make_async_copy(weight, scale, scale_sem)
    scale_copy.start()
    scale_copy.wait()
    for index in range(2 * early):
        sums[index] = hermitian(ahead[index], scale[...])
    for pair in range(late):
        copies[pair].wait()
        for index in range(2 * pair, 2 * pair + 2):
            sums[2 * early + index] = hermitian(rest[index], scale[...])


def gram_other(spectra, weight):
    groups, points, width = spectra.shape
    half = width // 2
    return pl.pallas_call(
        gram_other_kernel,
        in_specs=[HBM, HBM],
        out_specs=(VMEM, VMEM, VMEM),
        out_shape=(
            jax.ShapeDtypeStruct((groups // 2, half, half), F32),
            pltpu.VMEM((groups // 2, points, width), BF16),
            pltpu.VMEM((groups // 4, points, width), BF16),
        ),
        scratch_shapes=[
            pltpu.VMEM((1, points), F32),
            pltpu.SemaphoreType.DMA((groups // 4,)),
            pltpu.SemaphoreType.DMA((groups // 8,)),
            pltpu.SemaphoreType.DMA,
        ],
        compiler_params=kernel_params(16),
        cost_estimate=cost(groups * points * width * width, groups * points * width),
        name="gram_other",
    )(spectra, weight)


def gram_mine(ahead, spectra, weight):
    groups, points, width = spectra.shape
    half = width // 2
    return pl.pallas_call(
        gram_mine_kernel,
        in_specs=[VMEM, HBM, HBM],
        out_specs=(VMEM, VMEM),
        out_shape=(
            jax.ShapeDtypeStruct((groups // 2, half, half), F32),
            pltpu.VMEM((groups // 4, points, width), BF16),
        ),
        scratch_shapes=[
            pltpu.VMEM((1, points), F32),
            pltpu.SemaphoreType.DMA((groups // 8,)),
            pltpu.SemaphoreType.DMA,
        ],
        compiler_params=kernel_params(16),
        cost_estimate=cost(groups * points * width * width, groups * points * width),
        name="gram_mine",
    )(ahead, spectra, weight)


def orthonormal(re, im):
    rows, _ = iotas(re.shape)
    for k in range(KMAX):
        ure = jnp.broadcast_to(re[k : k + 1], re.shape)
        uim = jnp.broadcast_to(im[k : k + 1], im.shape)
        square = jnp.sum(ure * ure + uim * uim, axis=1, keepdims=True) + EPS
        pre = jnp.sum(ure * re + uim * im, axis=1, keepdims=True)
        pim = jnp.sum(ure * im - uim * re, axis=1, keepdims=True)
        unit = lax.rsqrt(square)
        inverse = unit * unit
        pre = pre * inverse
        pim = pim * inverse
        re, im = (
            jnp.where(rows > k, re - pre * ure + pim * uim, jnp.where(rows == k, ure * unit, re)),
            jnp.where(rows > k, im - pre * uim - pim * ure, jnp.where(rows == k, uim * unit, im)),
        )
    return (re, im)


def solve_kernel(total, orders, parts, counts, partner, out, table, kept_all, partners, sems):
    count, half, _ = parts.shape
    small = (
        pltpu.make_async_copy(counts, kept_all, sems.at[0]),
        pltpu.make_async_copy(partner, partners, sems.at[1]),
    )
    for copy in small:
        copy.start()
    summed = parts[0].astype(F32)
    for index in range(1, count):
        summed = summed + parts[index].astype(F32)
    summed = summed / total
    flipped = summed.T
    rows, cols = iotas((half, half))
    gram_re = jnp.where(cols >= rows, summed, flipped)
    gram_im = jnp.where(cols < rows, summed, jnp.where(cols > rows, -flipped, 0.0))
    operator = jnp.concatenate(
        [
            jnp.concatenate([gram_re, -gram_im], axis=1),
            jnp.concatenate([gram_im, gram_re], axis=1),
        ],
        axis=0,
    )
    high = operator.astype(BF16)
    low = (operator - high.astype(F32)).astype(BF16)

    def apply(re, im):
        vectors = jnp.concatenate([re, im], axis=1)
        vhigh = vectors.astype(BF16)
        vlow = (vectors - vhigh.astype(F32)).astype(BF16)
        both = jnp.concatenate([vhigh, vlow], axis=0)
        first = jnp.dot(both, high, preferred_element_type=F32)
        second = jnp.dot(both, low, preferred_element_type=F32)
        image = first[:KMAX] + first[KMAX:] + second[:KMAX]
        return (image[:, :half], image[:, half:])

    re, im = orthonormal(gram_re[:KMAX], -gram_im[:KMAX])
    for _ in range(ITERS - 1):
        re, im = orthonormal(*apply(re, im))
    image_re, image_im = apply(re, im)
    energy = jnp.sum(re * image_re + im * image_im, axis=1, keepdims=True)
    for copy in small:
        copy.wait()
    place = lax.axis_index("space")
    z_high = lax.rem(lax.axis_index("freq"), 2)
    slot = jnp.int32(0)
    for side, order in enumerate(orders):
        for index, chip in enumerate(order):
            slot = jnp.where((z_high == side) & (place // 2 == chip), index, slot)
    kept = kept_all[lax.rem(place, 2) * (kept_all.shape[0] // 2) + slot]
    ranks, lanes = iotas((KMAX, half))
    scale = jnp.where(ranks[:, :1] < kept, 1.0 / jnp.sqrt(energy + EPS), 0.0)
    first = energy.astype(BF16)
    rest = energy - first.astype(F32)
    second = rest.astype(BF16)
    third = (rest - second.astype(F32)).astype(BF16)
    tail = jnp.where(
        lanes == 0,
        first.astype(F32),
        jnp.where(lanes == 1, second.astype(F32), jnp.where(lanes == 2, third.astype(F32), 0.0)),
    )
    message = jnp.concatenate([re * scale, im * scale, tail], axis=1).astype(BF16)
    for index in range(out.shape[0]):
        out[index] = message
    _, lanes = iotas(table.shape)
    value = jnp.zeros(table.shape, jnp.int32)
    for index in range(partners.shape[0]):
        value = jnp.where(lanes // (2 * KMAX) == index, partners[index], value)
    table[...] = value.astype(F32).astype(BF16)


def solve(parts, counts, partner, total, orders, lanes):
    _, half, _ = parts.shape
    groups = counts.shape[0]
    return pl.pallas_call(
        functools.partial(solve_kernel, total, orders),
        in_specs=[VMEM, HBM, HBM],
        out_specs=(VMEM, VMEM),
        out_shape=(
            jax.ShapeDtypeStruct((groups, KMAX, 3 * half), BF16),
            jax.ShapeDtypeStruct((2 * KMAX, lanes), BF16),
        ),
        scratch_shapes=[
            pltpu.SMEM((groups,), jnp.int32),
            pltpu.SMEM((groups,), jnp.int32),
            pltpu.SemaphoreType.DMA((2,)),
        ],
        compiler_params=kernel_params(8),
        cost_estimate=cost(8_000_000_000, parts.size * 2),
        name="solve",
    )(parts, counts, partner)


def place_of(index, groups):
    return 2 * (index % (groups // 2)) + 1 - index // (groups // 2)


def held_parts(theirs, ahead, rest):
    core = on_core()
    return ((theirs, 1 - core, 0), (ahead, core, 0), (rest, core, ahead.shape[0]))


def coefficient_rows(message, half):
    part_re = message[:, :half]
    part_im = message[:, half : 2 * half]
    return jnp.concatenate(
        [
            jnp.concatenate([part_re, -part_im], axis=1),
            jnp.concatenate([part_im, part_re], axis=1),
        ],
        axis=0,
    )


def project(rows, block):
    return lax.dot_general(
        rows, block, (((1,), (1,)), ((), ())), preferred_element_type=F32
    ).astype(BF16)


def part_kernel(begin, size, messages, table, theirs, ahead, rest, *more):
    out = more[-1]
    groups = messages.shape[0]
    _, points, width = theirs.shape
    start = pl.multiple_of((1 - kept_half()) * (points // 2) + begin, 128)
    for held, side, first in held_parts(theirs, ahead, rest):
        for index in range(held.shape[0]):
            rows = coefficient_rows(messages[2 * (first + index) + 1 - side], width // 2)
            target = side * (groups // 2) + first + index
            out[target] = project(rows, held[index, pl.ds(start, size)])
    if out.shape[0] > groups:
        out[groups] = table[...]


def modes_part(messages, table, held, begin, size, planes, *after):
    groups = messages.shape[0]
    width = held[0].shape[2]
    return pl.pallas_call(
        functools.partial(part_kernel, begin, size),
        in_specs=[VMEM] * 5 + [ANY] * len(after),
        out_specs=VMEM,
        out_shape=jax.ShapeDtypeStruct((planes, 2 * KMAX, size), BF16),
        compiler_params=kernel_params(8),
        cost_estimate=cost(2_000_000_000, groups * size * width * 2),
        name="modes_part",
    )(messages, table, *held, *after)


def modes_kernel(slots, messages, weight, theirs, ahead, rest, after, out, energy, high, low, made, put):
    groups = messages.shape[0]
    _, points, width = theirs.shape
    part = points // 2
    upper = kept_half() == 1
    scale = weight[:, pl.ds(pl.multiple_of(kept_half() * part, 128), part)]
    _, lanes = iotas(energy.shape)
    value = jnp.zeros(energy.shape, F32)
    for index in range(groups):
        column = jnp.sum(
            messages[place_of(index, groups), :, width:].astype(F32), axis=1, keepdims=True
        )
        value = jnp.where(lanes == index, column, value)
    energy[...] = value

    def store(slot, target):
        return pltpu.make_async_copy(made.at[slot], out.at[target], put.at[slot])

    done = 0
    for held, side, first in held_parts(theirs, ahead, rest):

        def body(turn, carry, held=held, side=side, first=first, done=done):
            local = [2 * turn, 2 * turn + 1]
            places = [lax.rem(done + index, slots) for index in local]
            targets = [side * (groups // 2) + first + index for index in local]
            for index, slot, target in zip(local, places, targets):

                @pl.when(done + index >= slots)
                def _():
                    store(slot, target).wait()

            for index, slot, target in zip(local, places, targets):
                rows = coefficient_rows(messages[2 * (first + index) + 1 - side], width // 2)
                value = project(rows, held[index])
                made[slot] = value
                own = jnp.where(upper, value[:, part:], value[:, :part]).astype(F32) * scale
                top = own.astype(BF16)
                high[target] = top
                low[target] = (own - top.astype(F32)).astype(BF16)
            for slot, target in zip(places, targets):
                store(slot, target).start()
            return carry

        lax.fori_loop(0, held.shape[0] // 2, body, 0)
        done += held.shape[0]
    for slot in range(slots):
        store(slot, slot).wait()


def modes_all(messages, weight, held, after):
    groups = messages.shape[0]
    _, points, width = held[0].shape
    slots = 4
    weighted = jax.ShapeDtypeStruct((groups, 2 * KMAX, points // 2), BF16)
    return pl.pallas_call(
        functools.partial(modes_kernel, slots),
        in_specs=[VMEM] * 5 + [ANY],
        out_specs=(HBM, VMEM, VMEM, VMEM),
        out_shape=(
            jax.ShapeDtypeStruct((groups, 2 * KMAX, points), BF16),
            jax.ShapeDtypeStruct((KMAX, groups), F32),
            weighted,
            weighted,
        ),
        scratch_shapes=[
            pltpu.VMEM((slots, 2 * KMAX, points), BF16),
            pltpu.SemaphoreType.DMA((slots,)),
        ],
        compiler_params=kernel_params(12),
        cost_estimate=cost(7_000_000_000, groups * points * width * 2),
        name="modes_all",
    )(messages, weight, *held, after)


def chosen(cross, lane_partner, groups):
    rank = 2 * KMAX
    top = jnp.zeros((KMAX, groups * rank), F32)
    bottom = jnp.zeros((KMAX, groups * rank), F32)
    for index in range(groups):
        taken = lane_partner == index
        top = jnp.where(taken, cross[index * rank : index * rank + KMAX], top)
        bottom = jnp.where(taken, cross[index * rank + KMAX : (index + 1) * rank], bottom)
    _, lanes = iotas(top.shape)
    width = groups * rank
    return jnp.where(
        lanes % rank < KMAX,
        top + pltpu.roll(bottom, width - KMAX, 1),
        pltpu.roll(bottom, KMAX, 1) - top,
    )


def products(high, low, share, begin):
    groups, rank, _ = high.shape
    rows, size = (groups * rank, share.shape[2])
    other = share[:groups].reshape(rows, size)
    total = None
    for own in (high, low):
        mine = own[:, :, begin : begin + size].reshape(rows, size)
        part = lax.dot_general(mine, other, (((1,), (1,)), ((), ())), preferred_element_type=F32)
        total = part if total is None else total + part
    return total


def early_kernel(begins, high, low, *rest):
    arrived, out = (rest[:-1], rest[-1])
    value = products(high, low, arrived[0], begins[0])
    for share, begin in zip(arrived[1:], begins[1:]):
        value = value + products(high, low, share, begin)
    out[...] = value


def early_products(high, low, arrived, begins):
    rows = high.shape[0] * high.shape[1]
    return pl.pallas_call(
        functools.partial(early_kernel, begins),
        in_specs=[VMEM] * (2 + len(arrived)),
        out_specs=VMEM,
        out_shape=jax.ShapeDtypeStruct((rows, rows), F32),
        compiler_params=kernel_params(8),
        cost_estimate=cost(2_000_000_000, 4 * high.size),
        name="early_products",
    )(high, low, *arrived)


def cross_kernel(begin, sides, early, table, high, low, share, out):
    groups, rank, part = high.shape
    rows = groups * rank
    cross = early[...] + products(high, low, share, begin)
    own_table = table[:KMAX, :rows].astype(F32).astype(jnp.int32)
    other_table = share[groups, :KMAX, :rows].astype(F32).astype(jnp.int32)
    own_value = chosen(cross.T, own_table, groups)
    other_value = chosen(cross, other_table, groups)
    both = jnp.concatenate([own_value, other_value], axis=0).astype(BF16)
    source, target = iotas((rows, rows))
    moved = target == (source % rank) * groups + source // rank
    ordered = jnp.dot(both, moved.astype(F32).astype(BF16), preferred_element_type=F32)
    own_copy = ordered[:KMAX].astype(BF16)
    other_copy = ordered[KMAX:].astype(BF16)
    place = lax.axis_index("freq")
    upper = kept_half()
    pair = jnp.where(upper == 0, place, lax.axis_size("freq") - 1 - place)
    step = 16
    for begin in range(0, out.shape[0], step):
        bits = jnp.int32(0)
        for index, side in enumerate(sides):
            mask = sum(bit << k for k, bit in enumerate(side[begin : begin + step]))
            bits = jnp.where(pair == index, mask, bits)
        for k in range(step):
            same = ((bits >> k) & 1) == upper
            out[begin + k] = jnp.where(same, own_copy, other_copy)


def cross_sums(early, table, high, low, share, begin, sides):
    groups, rank, part = high.shape
    members = len(sides[0])
    return pl.pallas_call(
        functools.partial(cross_kernel, begin, sides),
        in_specs=[VMEM] * 5,
        out_specs=VMEM,
        out_shape=jax.ShapeDtypeStruct((members, KMAX, groups * rank), BF16),
        compiler_params=kernel_params(8),
        cost_estimate=cost(2_000_000_000, 4 * high.size),
        name="cross_sums",
    )(early, table, high, low, share)


def finish_kernel(total, parts, out):
    summed = parts[0].astype(F32)
    for index in range(1, parts.shape[0]):
        summed = summed + parts[index].astype(F32)
    summed = summed / total
    groups = out.shape[3]
    for side in range(2):
        for k in range(KMAX):
            begin = (side * KMAX + k) * groups
            out[side, k] = summed[:, begin : begin + groups]


def finish(parts, total):
    _, kmax, width = parts.shape
    return pl.pallas_call(
        functools.partial(finish_kernel, total),
        in_specs=[VMEM],
        out_specs=VMEM,
        out_shape=jax.ShapeDtypeStruct((2, kmax, kmax, width // (2 * kmax)), F32),
        compiler_params=kernel_params(8),
        cost_estimate=cost(1_000_000, parts.size * 2),
        name="finish",
    )(parts)


def hops_from_corner(device, n_space):
    freq, space = divmod(device, n_space)
    x, z_high = divmod(freq, 2)
    z_low, rest = divmod(space, 8)
    return sum(min(a, 4 - a) for a in (x, rest // 2, 2 * z_high + z_low))


def on_device(spectra, weight, partner, counts):
    groups, points, width = spectra.shape
    n_freq, n_space = (lax.axis_size("freq"), lax.axis_size("space"))
    total = points * n_space
    spectra = pltpu.with_memory_space_constraint(spectra, pltpu.HBM)
    weight_row = weight[None, :]
    mirror = [(index, n_freq - 1 - index) for index in range(n_freq)]

    weight_hbm = pltpu.with_memory_space_constraint(weight_row, pltpu.HBM)
    other, theirs, ahead = gram_other(spectra, weight_hbm)
    swapped = lax.ppermute(other, "space", [(index, index ^ 1) for index in range(n_space)])
    ahead = pltpu.with_memory_space_constraint(ahead, pltpu.VMEM)
    mine, rest = gram_mine(ahead, spectra, weight_hbm)
    held = [
        pltpu.with_memory_space_constraint(theirs, pltpu.VMEM),
        ahead,
        pltpu.with_memory_space_constraint(rest, pltpu.VMEM),
    ]
    orders = [
        sorted(range(n_space // 2), key=lambda chip: -hops_from_corner(side * n_space + 2 * chip, n_space))
        for side in range(2)
    ]
    both_axes = ("freq", "space")
    chips = [
        [group * n_space + 2 * chip + core for chip in orders[group % 2]]
        for group in range(n_freq)
        for core in range(2)
    ]
    devices = [
        [group * n_space + 2 * chip + core for chip in orders[group % 2] for core in (1, 0)]
        for group in range(n_freq)
    ]
    parts = lax.all_to_all(
        (mine + swapped).astype(BF16), both_axes, 0, 0, tiled=True, axis_index_groups=chips
    )
    part = points // 2
    sizes = (part // 4, part // 2, part // 4)
    begins = (0, part // 4, 3 * part // 4)
    in_hbm = [pltpu.with_memory_space_constraint(array, pltpu.HBM) for array in (counts, partner)]
    message, table = solve(parts, *in_hbm, total, orders, sizes[-1])
    messages = lax.all_to_all(
        message, both_axes, 0, 0, tiled=True, axis_index_groups=devices
    )

    shares = []
    for begin, size in zip(begins, sizes):
        planes = groups + 1 if size + begin == part else groups
        shares.append(modes_part(messages, table, held, begin, size, planes, *shares[-1:]))
    arrived = [lax.ppermute(share, "freq", mirror) for share in shares]
    modes, energy, high, low = modes_all(messages, weight_row, held, shares[-1])
    early = early_products(high, low, arrived[:-1], begins[:-1])

    members = [
        sorted(
            (group * n_space + index for group in (low_group, n_freq - 1 - low_group) for index in range(n_space)),
            key=lambda device: -hops_from_corner(device, n_space),
        )
        for low_group in range(n_freq // 2)
    ]
    sides = [[2 * device // (n_freq * n_space) for device in order] for order in members]
    gathered = lax.all_to_all(
        cross_sums(
            early, table, high, low, arrived[-1], begins[-1], sides
        ),
        both_axes,
        0,
        0,
        tiled=True,
        axis_index_groups=members,
    )
    coherence = jnp.transpose(finish(gathered, total), (3, 0, 1, 2))
    return (modes, jnp.transpose(energy), coherence)


def solution(mesh):
    in_specs = (P("freq", "space", None), P("space"), P("freq"), P("freq"))
    out_specs = (P("freq", None, "space"), P("freq", None), P("freq", None, None, None))
    return jax.shard_map(
        on_device, mesh=mesh, in_specs=in_specs, out_specs=out_specs, check_vma=False
    )
```

```python
import functools

import jax
import jax.numpy as jnp
from jax import lax
from jax.experimental import pallas as pl
from jax.experimental.pallas import tpu as pltpu
from jax.sharding import PartitionSpec as P

KMAX = 8
ITERS = 4
EPS = 1e-06
F32 = jnp.float32
BF16 = jnp.bfloat16
VMEM = pl.BlockSpec(memory_space=pltpu.VMEM)
SMEM = pl.BlockSpec(memory_space=pltpu.SMEM)
ANY = pl.BlockSpec(memory_space=pl.ANY)
HBM = pl.BlockSpec(memory_space=pltpu.HBM)


def kernel_params(mebibytes):
    return pltpu.CompilerParams(vmem_limit_bytes=mebibytes * 1024 * 1024)


def cost(flops, moved):
    return pl.CostEstimate(flops=flops, bytes_accessed=moved, transcendentals=0)


def kept_half():
    return jnp.where(lax.axis_index("freq") < lax.axis_size("freq") // 2, 0, 1)


def iotas(shape):
    return (
        lax.broadcasted_iota(jnp.int32, shape, 0),
        lax.broadcasted_iota(jnp.int32, shape, 1),
    )


def hermitian(block, scale):
    half = block.shape[1] // 2
    rows, cols = iotas((half, half))
    weighted = (block.T.astype(F32) * scale).astype(BF16)
    moment = jnp.dot(weighted, block, preferred_element_type=F32)
    real = moment[:half, :half] + moment[half:, half:]
    imag = moment[:half, half:] - moment[half:, :half]
    return jnp.where(cols >= rows, real, imag)


def on_core():
    return lax.rem(lax.axis_index("space"), 2)


def pair_copy(spectra, held, sems, side, pair, slot):
    begin = side * (spectra.shape[0] // 2) + 2 * pair
    return pltpu.make_async_copy(
        spectra.at[pl.ds(begin, 2)], held.at[pl.ds(2 * slot, 2)], sems.at[slot]
    )


def gram_other_kernel(spectra, weight, sums, theirs, ahead, scale, sems, ahead_sems, scale_sem):
    pairs = theirs.shape[0] // 2
    early = ahead.shape[0] // 2
    copies = [pair_copy(spectra, theirs, sems, 1 - on_core(), p, p) for p in range(pairs)]
    copies += [pair_copy(spectra, ahead, ahead_sems, on_core(), p, p) for p in range(early)]
    due = {0: (2, 3), 1: (4,), 2: (5,)}
    copies[0].start()
    scale_copy = pltpu.make_async_copy(weight, scale, scale_sem)
    scale_copy.start()
    copies[1].start()
    scale_copy.wait()
    for pair in range(pairs):
        copies[pair].wait()
        for later in due.get(pair, ()):
            copies[later].start()
        for index in range(2 * pair, 2 * pair + 2):
            sums[index] = hermitian(theirs[index], scale[...])
    for copy in copies[pairs:]:
        copy.wait()


def gram_mine_kernel(ahead, spectra, weight, sums, rest, scale, sems, scale_sem):
    early, late = (ahead.shape[0] // 2, rest.shape[0] // 2)
    copies = [pair_copy(spectra, rest, sems, on_core(), early + p, p) for p in range(late)]
    for copy in copies:
        copy.start()
    scale_copy = pltpu.make_async_copy(weight, scale, scale_sem)
    scale_copy.start()
    scale_copy.wait()
    for index in range(2 * early):
        sums[index] = hermitian(ahead[index], scale[...])
    for pair in range(late):
        copies[pair].wait()
        for index in range(2 * pair, 2 * pair + 2):
            sums[2 * early + index] = hermitian(rest[index], scale[...])


def gram_other(spectra, weight):
    groups, points, width = spectra.shape
    half = width // 2
    return pl.pallas_call(
        gram_other_kernel,
        in_specs=[HBM, HBM],
        out_specs=(VMEM, VMEM, VMEM),
        out_shape=(
            jax.ShapeDtypeStruct((groups // 2, half, half), F32),
            pltpu.VMEM((groups // 2, points, width), BF16),
            pltpu.VMEM((groups // 4, points, width), BF16),
        ),
        scratch_shapes=[
            pltpu.VMEM((1, points), F32),
            pltpu.SemaphoreType.DMA((groups // 4,)),
            pltpu.SemaphoreType.DMA((groups // 8,)),
            pltpu.SemaphoreType.DMA,
        ],
        compiler_params=kernel_params(16),
        cost_estimate=cost(groups * points * width * width, groups * points * width),
        name="gram_other",
    )(spectra, weight)


def gram_mine(ahead, spectra, weight):
    groups, points, width = spectra.shape
    half = width // 2
    return pl.pallas_call(
        gram_mine_kernel,
        in_specs=[VMEM, HBM, HBM],
        out_specs=(VMEM, VMEM),
        out_shape=(
            jax.ShapeDtypeStruct((groups // 2, half, half), F32),
            pltpu.VMEM((groups // 4, points, width), BF16),
        ),
        scratch_shapes=[
            pltpu.VMEM((1, points), F32),
            pltpu.SemaphoreType.DMA((groups // 8,)),
            pltpu.SemaphoreType.DMA,
        ],
        compiler_params=kernel_params(16),
        cost_estimate=cost(groups * points * width * width, groups * points * width),
        name="gram_mine",
    )(ahead, spectra, weight)


def orthonormal(re, im):
    rows, _ = iotas(re.shape)
    for k in range(KMAX):
        ure = jnp.broadcast_to(re[k : k + 1], re.shape)
        uim = jnp.broadcast_to(im[k : k + 1], im.shape)
        square = jnp.sum(ure * ure + uim * uim, axis=1, keepdims=True) + EPS
        pre = jnp.sum(ure * re + uim * im, axis=1, keepdims=True)
        pim = jnp.sum(ure * im - uim * re, axis=1, keepdims=True)
        unit = lax.rsqrt(square)
        inverse = unit * unit
        pre = pre * inverse
        pim = pim * inverse
        re, im = (
            jnp.where(rows > k, re - pre * ure + pim * uim, jnp.where(rows == k, ure * unit, re)),
            jnp.where(rows > k, im - pre * uim - pim * ure, jnp.where(rows == k, uim * unit, im)),
        )
    return (re, im)


def solve_kernel(total, orders, parts, counts, partner, out, table, kept_all, partners, sems):
    count, half, _ = parts.shape
    small = (
        pltpu.make_async_copy(counts, kept_all, sems.at[0]),
        pltpu.make_async_copy(partner, partners, sems.at[1]),
    )
    for copy in small:
        copy.start()
    summed = parts[0].astype(F32)
    for index in range(1, count):
        summed = summed + parts[index].astype(F32)
    summed = summed / total
    flipped = summed.T
    rows, cols = iotas((half, half))
    gram_re = jnp.where(cols >= rows, summed, flipped)
    gram_im = jnp.where(cols < rows, summed, jnp.where(cols > rows, -flipped, 0.0))
    operator = jnp.concatenate(
        [
            jnp.concatenate([gram_re, -gram_im], axis=1),
            jnp.concatenate([gram_im, gram_re], axis=1),
        ],
        axis=0,
    )
    high = operator.astype(BF16)
    low = (operator - high.astype(F32)).astype(BF16)

    def apply(re, im):
        vectors = jnp.concatenate([re, im], axis=1)
        vhigh = vectors.astype(BF16)
        vlow = (vectors - vhigh.astype(F32)).astype(BF16)
        both = jnp.concatenate([vhigh, vlow], axis=0)
        first = jnp.dot(both, high, preferred_element_type=F32)
        second = jnp.dot(both, low, preferred_element_type=F32)
        image = first[:KMAX] + first[KMAX:] + second[:KMAX]
        return (image[:, :half], image[:, half:])

    re, im = orthonormal(gram_re[:KMAX], -gram_im[:KMAX])
    for _ in range(ITERS - 1):
        re, im = orthonormal(*apply(re, im))
    image_re, image_im = apply(re, im)
    energy = jnp.sum(re * image_re + im * image_im, axis=1, keepdims=True)
    for copy in small:
        copy.wait()
    place = lax.axis_index("space")
    z_high = lax.rem(lax.axis_index("freq"), 2)
    slot = jnp.int32(0)
    for side, order in enumerate(orders):
        for index, chip in enumerate(order):
            slot = jnp.where((z_high == side) & (place // 2 == chip), index, slot)
    kept = kept_all[lax.rem(place, 2) * (kept_all.shape[0] // 2) + slot]
    ranks, lanes = iotas((KMAX, half))
    scale = jnp.where(ranks[:, :1] < kept, 1.0 / jnp.sqrt(energy + EPS), 0.0)
    first = energy.astype(BF16)
    rest = energy - first.astype(F32)
    second = rest.astype(BF16)
    third = (rest - second.astype(F32)).astype(BF16)
    tail = jnp.where(
        lanes == 0,
        first.astype(F32),
        jnp.where(lanes == 1, second.astype(F32), jnp.where(lanes == 2, third.astype(F32), 0.0)),
    )
    message = jnp.concatenate([re * scale, im * scale, tail], axis=1).astype(BF16)
    for index in range(out.shape[0]):
        out[index] = message
    _, lanes = iotas(table.shape)
    value = jnp.zeros(table.shape, jnp.int32)
    for index in range(partners.shape[0]):
        value = jnp.where(lanes // (2 * KMAX) == index, partners[index], value)
    table[...] = value.astype(F32).astype(BF16)


def solve(parts, counts, partner, total, orders, lanes):
    _, half, _ = parts.shape
    groups = counts.shape[0]
    return pl.pallas_call(
        functools.partial(solve_kernel, total, orders),
        in_specs=[VMEM, HBM, HBM],
        out_specs=(VMEM, VMEM),
        out_shape=(
            jax.ShapeDtypeStruct((groups, KMAX, 3 * half), BF16),
            jax.ShapeDtypeStruct((2 * KMAX, lanes), BF16),
        ),
        scratch_shapes=[
            pltpu.SMEM((groups,), jnp.int32),
            pltpu.SMEM((groups,), jnp.int32),
            pltpu.SemaphoreType.DMA((2,)),
        ],
        compiler_params=kernel_params(8),
        cost_estimate=cost(8_000_000_000, parts.size * 2),
        name="solve",
    )(parts, counts, partner)


def place_of(index, groups):
    return 2 * (index % (groups // 2)) + 1 - index // (groups // 2)


def held_parts(theirs, ahead, rest):
    core = on_core()
    return ((theirs, 1 - core, 0), (ahead, core, 0), (rest, core, ahead.shape[0]))


def coefficient_rows(message, half):
    part_re = message[:, :half]
    part_im = message[:, half : 2 * half]
    return jnp.concatenate(
        [
            jnp.concatenate([part_re, -part_im], axis=1),
            jnp.concatenate([part_im, part_re], axis=1),
        ],
        axis=0,
    )


def project(rows, block):
    return lax.dot_general(
        rows, block, (((1,), (1,)), ((), ())), preferred_element_type=F32
    ).astype(BF16)


def part_kernel(begin, size, messages, table, theirs, ahead, rest, *more):
    out = more[-1]
    groups = messages.shape[0]
    _, points, width = theirs.shape
    start = pl.multiple_of((1 - kept_half()) * (points // 2) + begin, 128)
    for held, side, first in held_parts(theirs, ahead, rest):
        for index in range(held.shape[0]):
            rows = coefficient_rows(messages[2 * (first + index) + 1 - side], width // 2)
            target = side * (groups // 2) + first + index
            out[target] = project(rows, held[index, pl.ds(start, size)])
    if out.shape[0] > groups:
        out[groups] = table[...]


def modes_part(messages, table, held, begin, size, planes, *after):
    groups = messages.shape[0]
    width = held[0].shape[2]
    return pl.pallas_call(
        functools.partial(part_kernel, begin, size),
        in_specs=[VMEM] * 5 + [ANY] * len(after),
        out_specs=VMEM,
        out_shape=jax.ShapeDtypeStruct((planes, 2 * KMAX, size), BF16),
        compiler_params=kernel_params(8),
        cost_estimate=cost(2_000_000_000, groups * size * width * 2),
        name="modes_part",
    )(messages, table, *held, *after)


def modes_kernel(slots, messages, weight, theirs, ahead, rest, after, out, energy, high, low, made, put):
    groups = messages.shape[0]
    _, points, width = theirs.shape
    part = points // 2
    upper = kept_half() == 1
    scale = weight[:, pl.ds(pl.multiple_of(kept_half() * part, 128), part)]
    _, lanes = iotas(energy.shape)
    value = jnp.zeros(energy.shape, F32)
    for index in range(groups):
        column = jnp.sum(
            messages[place_of(index, groups), :, width:].astype(F32), axis=1, keepdims=True
        )
        value = jnp.where(lanes == index, column, value)
    energy[...] = value

    def store(slot, target):
        return pltpu.make_async_copy(made.at[slot], out.at[target], put.at[slot])

    done = 0
    for held, side, first in held_parts(theirs, ahead, rest):

        def body(turn, carry, held=held, side=side, first=first, done=done):
            local = [2 * turn, 2 * turn + 1]
            places = [lax.rem(done + index, slots) for index in local]
            targets = [side * (groups // 2) + first + index for index in local]
            for index, slot, target in zip(local, places, targets):

                @pl.when(done + index >= slots)
                def _():
                    store(slot, target).wait()

            for index, slot, target in zip(local, places, targets):
                rows = coefficient_rows(messages[2 * (first + index) + 1 - side], width // 2)
                value = project(rows, held[index])
                made[slot] = value
                own = jnp.where(upper, value[:, part:], value[:, :part]).astype(F32) * scale
                top = own.astype(BF16)
                high[target] = top
                low[target] = (own - top.astype(F32)).astype(BF16)
            for slot, target in zip(places, targets):
                store(slot, target).start()
            return carry

        lax.fori_loop(0, held.shape[0] // 2, body, 0)
        done += held.shape[0]
    for slot in range(slots):
        store(slot, slot).wait()


def modes_all(messages, weight, held, after):
    groups = messages.shape[0]
    _, points, width = held[0].shape
    slots = 4
    weighted = jax.ShapeDtypeStruct((groups, 2 * KMAX, points // 2), BF16)
    return pl.pallas_call(
        functools.partial(modes_kernel, slots),
        in_specs=[VMEM] * 5 + [ANY],
        out_specs=(HBM, VMEM, VMEM, VMEM),
        out_shape=(
            jax.ShapeDtypeStruct((groups, 2 * KMAX, points), BF16),
            jax.ShapeDtypeStruct((KMAX, groups), F32),
            weighted,
            weighted,
        ),
        scratch_shapes=[
            pltpu.VMEM((slots, 2 * KMAX, points), BF16),
            pltpu.SemaphoreType.DMA((slots,)),
        ],
        compiler_params=kernel_params(12),
        cost_estimate=cost(7_000_000_000, groups * points * width * 2),
        name="modes_all",
    )(messages, weight, *held, after)


def chosen(cross, lane_partner, groups):
    rank = 2 * KMAX
    top = jnp.zeros((KMAX, groups * rank), F32)
    bottom = jnp.zeros((KMAX, groups * rank), F32)
    for index in range(groups):
        taken = lane_partner == index
        top = jnp.where(taken, cross[index * rank : index * rank + KMAX], top)
        bottom = jnp.where(taken, cross[index * rank + KMAX : (index + 1) * rank], bottom)
    _, lanes = iotas(top.shape)
    width = groups * rank
    return jnp.where(
        lanes % rank < KMAX,
        top + pltpu.roll(bottom, width - KMAX, 1),
        pltpu.roll(bottom, KMAX, 1) - top,
    )


def products(high, low, share, begin):
    groups, rank, _ = high.shape
    rows, size = (groups * rank, share.shape[2])
    other = share[:groups].reshape(rows, size)
    total = None
    for own in (high, low):
        mine = own[:, :, begin : begin + size].reshape(rows, size)
        part = lax.dot_general(mine, other, (((1,), (1,)), ((), ())), preferred_element_type=F32)
        total = part if total is None else total + part
    return total


def early_kernel(begins, high, low, *rest):
    arrived, out = (rest[:-1], rest[-1])
    value = products(high, low, arrived[0], begins[0])
    for share, begin in zip(arrived[1:], begins[1:]):
        value = value + products(high, low, share, begin)
    out[...] = value


def early_products(high, low, arrived, begins):
    rows = high.shape[0] * high.shape[1]
    return pl.pallas_call(
        functools.partial(early_kernel, begins),
        in_specs=[VMEM] * (2 + len(arrived)),
        out_specs=VMEM,
        out_shape=jax.ShapeDtypeStruct((rows, rows), F32),
        compiler_params=kernel_params(8),
        cost_estimate=cost(2_000_000_000, 4 * high.size),
        name="early_products",
    )(high, low, *arrived)


def cross_kernel(begin, sides, early, table, high, low, share, out):
    groups, rank, part = high.shape
    rows = groups * rank
    cross = early[...] + products(high, low, share, begin)
    own_table = table[:KMAX, :rows].astype(F32).astype(jnp.int32)
    other_table = share[groups, :KMAX, :rows].astype(F32).astype(jnp.int32)
    own_value = chosen(cross.T, own_table, groups)
    other_value = chosen(cross, other_table, groups)
    both = jnp.concatenate([own_value, other_value], axis=0).astype(BF16)
    source, target = iotas((rows, rows))
    moved = target == (source % rank) * groups + source // rank
    ordered = jnp.dot(both, moved.astype(F32).astype(BF16), preferred_element_type=F32)
    own_copy = ordered[:KMAX].astype(BF16)
    other_copy = ordered[KMAX:].astype(BF16)
    place = lax.axis_index("freq")
    upper = kept_half()
    pair = jnp.where(upper == 0, place, lax.axis_size("freq") - 1 - place)
    step = 16
    for begin in range(0, out.shape[0], step):
        bits = jnp.int32(0)
        for index, side in enumerate(sides):
            mask = sum(bit << k for k, bit in enumerate(side[begin : begin + step]))
            bits = jnp.where(pair == index, mask, bits)
        for k in range(step):
            same = ((bits >> k) & 1) == upper
            out[begin + k] = jnp.where(same, own_copy, other_copy)


def cross_sums(early, table, high, low, share, begin, sides):
    groups, rank, part = high.shape
    members = len(sides[0])
    return pl.pallas_call(
        functools.partial(cross_kernel, begin, sides),
        in_specs=[VMEM] * 5,
        out_specs=VMEM,
        out_shape=jax.ShapeDtypeStruct((members, KMAX, groups * rank), BF16),
        compiler_params=kernel_params(8),
        cost_estimate=cost(2_000_000_000, 4 * high.size),
        name="cross_sums",
    )(early, table, high, low, share)


def finish_kernel(total, parts, out):
    summed = parts[0].astype(F32)
    for index in range(1, parts.shape[0]):
        summed = summed + parts[index].astype(F32)
    summed = summed / total
    groups = out.shape[3]
    for side in range(2):
        for k in range(KMAX):
            begin = (side * KMAX + k) * groups
            out[side, k] = summed[:, begin : begin + groups]


def finish(parts, total):
    _, kmax, width = parts.shape
    return pl.pallas_call(
        functools.partial(finish_kernel, total),
        in_specs=[VMEM],
        out_specs=VMEM,
        out_shape=jax.ShapeDtypeStruct((2, kmax, kmax, width // (2 * kmax)), F32),
        compiler_params=kernel_params(8),
        cost_estimate=cost(1_000_000, parts.size * 2),
        name="finish",
    )(parts)


def hops_from_corner(device, n_space):
    freq, space = divmod(device, n_space)
    x, z_high = divmod(freq, 2)
    z_low, rest = divmod(space, 8)
    return sum(min(a, 4 - a) for a in (x, rest // 2, 2 * z_high + z_low))


def on_device(spectra, weight, partner, counts):
    groups, points, width = spectra.shape
    n_freq, n_space = (lax.axis_size("freq"), lax.axis_size("space"))
    total = points * n_space
    spectra = pltpu.with_memory_space_constraint(spectra, pltpu.HBM)
    weight_row = weight[None, :]
    mirror = [(index, n_freq - 1 - index) for index in range(n_freq)]

    weight_hbm = pltpu.with_memory_space_constraint(weight_row, pltpu.HBM)
    other, theirs, ahead = gram_other(spectra, weight_hbm)
    swapped = lax.ppermute(other, "space", [(index, index ^ 1) for index in range(n_space)])
    ahead = pltpu.with_memory_space_constraint(ahead, pltpu.VMEM)
    mine, rest = gram_mine(ahead, spectra, weight_hbm)
    held = [
        pltpu.with_memory_space_constraint(theirs, pltpu.VMEM),
        ahead,
        pltpu.with_memory_space_constraint(rest, pltpu.VMEM),
    ]
    orders = [
        sorted(range(n_space // 2), key=lambda chip: -hops_from_corner(side * n_space + 2 * chip, n_space))
        for side in range(2)
    ]
    both_axes = ("freq", "space")
    chips = [
        [group * n_space + 2 * chip + core for chip in orders[group % 2]]
        for group in range(n_freq)
        for core in range(2)
    ]
    devices = [
        [group * n_space + 2 * chip + core for chip in orders[group % 2] for core in (1, 0)]
        for group in range(n_freq)
    ]
    parts = lax.all_to_all(
        (mine + swapped).astype(BF16), both_axes, 0, 0, tiled=True, axis_index_groups=chips
    )
    part = points // 2
    sizes = (part // 3, part // 12 * 5, part // 4)
    begins = (0, part // 3, 3 * part // 4)
    in_hbm = [pltpu.with_memory_space_constraint(array, pltpu.HBM) for array in (counts, partner)]
    message, table = solve(parts, *in_hbm, total, orders, sizes[-1])
    messages = lax.all_to_all(
        message, both_axes, 0, 0, tiled=True, axis_index_groups=devices
    )

    shares = []
    for begin, size in zip(begins, sizes):
        planes = groups + 1 if size + begin == part else groups
        shares.append(modes_part(messages, table, held, begin, size, planes, *shares[-1:]))
    arrived = [lax.ppermute(share, "freq", mirror) for share in shares]
    modes, energy, high, low = modes_all(messages, weight_row, held, shares[-1])
    early = early_products(high, low, arrived[:-1], begins[:-1])

    members = [
        sorted(
            (group * n_space + index for group in (low_group, n_freq - 1 - low_group) for index in range(n_space)),
            key=lambda device: (-hops_from_corner(device, n_space), -(device % 2)),
        )
        for low_group in range(n_freq // 2)
    ]
    sides = [[2 * device // (n_freq * n_space) for device in order] for order in members]
    gathered = lax.all_to_all(
        cross_sums(
            early, table, high, low, arrived[-1], begins[-1], sides
        ),
        both_axes,
        0,
        0,
        tiled=True,
        axis_index_groups=members,
    )
    coherence = jnp.transpose(finish(gathered, total), (3, 0, 1, 2))
    return (modes, jnp.transpose(energy), coherence)


def solution(mesh):
    in_specs = (P("freq", "space", None), P("space"), P("freq"), P("freq"))
    out_specs = (P("freq", None, "space"), P("freq", None), P("freq", None, None, None))
    return jax.shard_map(
        on_device, mesh=mesh, in_specs=in_specs, out_specs=out_specs, check_vma=False
    )
```
